32 devices in a mesh: depth: 2 (over core), rows: 4 (over y, x), cols: 4 (over z).
Axes of the slice: x: 2, y: 2, z: 4, core: 2. Of those that a mesh axis runs over, the one named last changes fastest.
Arguments:
- section_states: float32 [2, 128, 64, 256], P('depth', 'rows', 'cols'), may hold values from -6 to 6
- weights: bfloat16 [4, 3, 3, 256, 256], P('depth'), may hold values from -0.125 to 0.125
Outputs:
- fine_states: float32 [4, 128, 64, 256], P('depth', 'rows', 'cols')
- coarse_states: float32 [2, 128, 64, 256], P('depth', 'rows', 'cols')
The draws below stay inside these ranges and needn't reach their ends.
All inputs are finite; a program needn't handle non-finite values.
Results may differ from the reference program's by a relative error of at most 0.002.
Values may be sent and summed in bfloat16 or wider, within the bound.
A program may use at most 64 MiB of HBM per device.

```python
import jax
import jax.numpy as jnp
from jax import lax

C = 256
SECTIONS = 2
LAYERS = 4
HEIGHT = 128
WIDTH = 64


def level_of(rng, extent, cuts, least, high):
    loudness, own = 1.0, jax.random.fold_in(rng, 6)
    for dim, blocks in cuts:
        steps = jnp.exp(jax.random.uniform(jax.random.fold_in(own, dim), (blocks,), jnp.float32, least / len(cuts), high / len(cuts)))
        loudness = loudness * jnp.repeat(steps, extent[dim] // blocks).reshape([-1 if axis == dim else 1 for axis in range(len(extent))])
    return loudness


def gaussian(rng, extent, scale, reach, shards=(), held_as=jnp.bfloat16):
    drawn = jax.random.normal(rng, extent, jnp.float32) * scale
    if len(shards) > 0:
        drawn = level_of(rng, extent, shards, -0.22, 0.18) * drawn
    return jnp.clip(drawn, min=-reach, max=reach).astype(held_as)


def setup_inputs(seed: int = 0) -> dict:
    splits = jax.random.split(jax.random.key(seed), 3)
    section_states = gaussian(splits[0], (SECTIONS, HEIGHT, WIDTH, C), 1.0, 6.0, ((0, 2), (1, 4), (2, 4)), jnp.float32)
    weights = gaussian(splits[1], (LAYERS, 3, 3, C, C), (9 * C) ** -0.5, 0.125, ((0, 2),))
    return dict(section_states=section_states, weights=weights)


def velocity(field, kernel):
    rows_here, cols_here, channels = field.shape
    rounded = lax.optimization_barrier(jax.nn.silu(field).astype(jnp.bfloat16)).astype(jnp.float32)
    padded = jnp.pad(rounded, ((1, 1), (1, 1), (0, 0)))
    summed = jnp.zeros((rows_here * cols_here, channels), jnp.float32)
    for shift_row in range(3):
        for shift_col in range(3):
            window = padded[shift_row:shift_row + rows_here, shift_col:shift_col + cols_here].reshape(-1, channels)
            summed = summed + jnp.dot(window, kernel[shift_row, shift_col].astype(jnp.float32), preferred_element_type=jnp.float32)
    return summed.reshape(rows_here, cols_here, channels)


def reference(section_states, weights):
    step_size = 2.0 / LAYERS
    sections = section_states.shape[0]
    jump_list = []
    for section in range(sections):
        anchor = section_states[section]
        first_slope = velocity(anchor, weights[2 * section])
        middle = anchor + step_size * first_slope
        ending = middle + step_size * velocity(middle, weights[2 * section + 1])
        jump_list.append(ending - (anchor + 2.0 * step_size * first_slope))
    coarse = [section_states[0]]
    for section in range(sections - 1):
        current = coarse[-1]
        coarse.append(current + 2.0 * step_size * velocity(current, weights[2 * section]) + jump_list[section])
    fine_list = []
    for section in range(sections):
        middle = coarse[section] + step_size * velocity(coarse[section], weights[2 * section])
        ending = middle + step_size * velocity(middle, weights[2 * section + 1])
        fine_list.append(middle)
        fine_list.append(ending)
    return jnp.stack(fine_list), jnp.stack(coarse)
```

```python
import functools

import jax
import jax.numpy as jnp
from jax import lax
from jax.experimental import pallas as pl
from jax.experimental.pallas import tpu as pltpu
from jax.sharding import PartitionSpec as P

MESH = pl.DeviceIdType.MESH
HALO = 4
LANES = 128


def padded_2(shard, sides, width):
    for axis, dim in sides:
        size, length = (lax.axis_size(axis), shard.shape[dim])
        up = [(i, (i + 1) % size) for i in range(size - 1)]
        down = [(j, i) for i, j in up]
        last = lax.slice_in_dim(shard, length - width, length, axis=dim)
        initial = lax.slice_in_dim(shard, 0, width, axis=dim)
        before = lax.ppermute(last, axis, up)
        after = lax.ppermute(initial, axis, down)
        shard = jnp.concatenate([before, shard, after], axis=dim)
    return shard


def shifted_2(block, axis, distance):
    devices = range(lax.axis_size(axis))
    route = [(i - distance, i) for i in devices if i - distance in devices]
    return lax.ppermute(block, axis, route)


def activate(field):
    return jax.nn.silu(field).astype(jnp.bfloat16)


def apply_stencil(padded, flat_weight, out_rows, out_cols):
    channels = padded.shape[2]
    patches = jnp.concatenate(
        [
            padded[shift_row : shift_row + out_rows, shift_col : shift_col + out_cols]
            for shift_row in range(3)
            for shift_col in range(3)
        ],
        axis=2,
    )
    summed = jnp.dot(
        patches.reshape(out_rows * out_cols, 9 * channels),
        flat_weight,
        preferred_element_type=jnp.float32,
    )
    return summed.reshape(out_rows, out_cols, channels)


def section_pass(anchor, first_weight, second_weight, step_size):
    rows_here, cols_here, channels = anchor.shape
    widened = padded_2(anchor, (("rows", 0), ("cols", 1)), 2)
    slope_wide = apply_stencil(activate(widened), first_weight, rows_here + 2, cols_here + 2)
    middle_wide = widened[1:-1, 1:-1] + step_size * slope_wide
    row_global = lax.axis_index("rows") * rows_here - 1 + jnp.arange(rows_here + 2)
    col_global = lax.axis_index("cols") * cols_here - 1 + jnp.arange(cols_here + 2)
    inside_rows = (row_global >= 0) & (row_global < rows_here * lax.axis_size("rows"))
    inside_cols = (col_global >= 0) & (col_global < cols_here * lax.axis_size("cols"))
    inside = inside_rows[:, None] & inside_cols[None, :]
    second_act = jnp.where(inside[:, :, None], activate(middle_wide), jnp.zeros((), jnp.bfloat16))
    first_slope = slope_wide[1:-1, 1:-1]
    middle = middle_wide[1:-1, 1:-1]
    second_slope = apply_stencil(second_act, second_weight, rows_here, cols_here)
    ending = middle + step_size * second_slope
    return (first_slope, middle, ending)


def chain_on_device(section_states, weights):
    rows_here, cols_here, channels = section_states.shape[1:]
    ndepth = lax.axis_size("depth")
    position = lax.axis_index("depth")
    step_size = 2.0 / (2 * ndepth)
    first_weight = weights[0].reshape(9 * channels, channels)
    second_weight = weights[1].reshape(9 * channels, channels)
    anchor = section_states[0]
    first_slope, middle, ending = section_pass(anchor, first_weight, second_weight, step_size)
    jump = ending - (anchor + 2.0 * step_size * first_slope)

    def chain_turn(step_index, current):
        padded = padded_2(activate(current), (("rows", 0), ("cols", 1)), 1)
        advanced = (
            current
            + 2.0 * step_size * apply_stencil(padded, first_weight, rows_here, cols_here)
            + jump
        )
        shifted = shifted_2(advanced, "depth", 1)
        return jnp.where(position == 0, anchor, shifted)

    corrected = lax.fori_loop(0, ndepth - 1, chain_turn, anchor)
    final_slope, final_middle, final_ending = section_pass(
        corrected, first_weight, second_weight, step_size
    )
    fine_states = jnp.stack([final_middle, final_ending])
    return (fine_states, corrected[None])


def largest_divisor(total, limit):
    return max(n for n in range(1, limit + 1) if total % n == 0)


DIRECTIONS = ((-1, 0), (1, 0), (0, -1), (0, 1), (-1, -1), (-1, 1), (1, -1), (1, 1))


def cycle_kernel(
    sizes, x_hbm, w_hbm, fine_hbm, coarse_hbm,
    x, w, base, mid, end, act0, act1, patches, stage,
    flat, send_row, send_col, recv_row, recv_col, recv_corner,
    load_sem, store_sem, send_sem, recv_sem, pass_send, pass_recv,
):
    nrows, ncols, step_size = sizes
    rows_here, cols_here, channels = x.shape
    halves = channels // LANES
    high, wide = rows_here + 2 * HALO, cols_here + 2 * HALO
    depth, row, col = lax.axis_index("depth"), lax.axis_index("rows"), lax.axis_index("cols")

    x_load = pltpu.make_async_copy(x_hbm.at[0], x, load_sem.at[0])
    w_loads = [pltpu.make_async_copy(w_hbm.at[k], w.at[k], load_sem.at[1 + k]) for k in range(2)]

    barrier = pltpu.get_barrier_semaphore()

    def neighbour(step):
        there_row, there_col = row + step[0], col + step[1]
        exists = (there_row >= 0) & (there_row < nrows) & (there_col >= 0) & (there_col < ncols)
        return exists, (depth, there_row, there_col)

    @pl.when(depth == 0)
    def _():
        x_load.start()

    for copy in w_loads:
        copy.start()
    pl.semaphore_signal(barrier, inc=1, device_id=(1 - depth, row, col), device_id_type=MESH)

    @pl.when(depth == 0)
    def _():
        for step in DIRECTIONS:
            exists, target = neighbour(step)

            @pl.when(exists)
            def _():
                pl.semaphore_signal(barrier, inc=1, device_id=target, device_id_type=MESH)

    def halves_of(c):
        return pl.ds(c * LANES, LANES)

    def masked_silu(u, first_row):
        n = u.shape[0]
        i = first_row + lax.broadcasted_iota(jnp.int32, (n, wide, LANES), 0) + (row * rows_here - HALO)
        j = lax.broadcasted_iota(jnp.int32, (n, wide, LANES), 1) + (col * cols_here - HALO)
        inside = (i >= 0) & (i < nrows * rows_here) & (j >= 0) & (j < ncols * cols_here)
        return jnp.where(inside, u / (1.0 + jnp.exp(-u)), 0.0)

    def slopes(act, layer, first_row, n, left, width):
        m = n * width
        for a in range(3):
            for b in range(3):
                for c in range(halves):
                    window = act[c, pl.ds(first_row + a - 1, n), left + b : left + b + width, :]
                    patches[0:m, pl.ds((a * 3 + b) * channels + c * LANES, LANES)] = (
                        window.reshape(m, LANES).astype(jnp.bfloat16)
                    )
        acc = jnp.dot(patches[0:m, :], w[layer], preferred_element_type=jnp.float32)
        return [
            step_size * acc[:, c * LANES : (c + 1) * LANES].reshape(n, width, LANES)
            for c in range(halves)
        ]

    def stage_interior(state, slot):
        def body(i, _):
            for c in range(halves):
                stage[slot, i, :, halves_of(c)] = state[c, i + HALO, HALO : HALO + cols_here, :]
            return 0

        lax.fori_loop(0, rows_here, body, 0, unroll=4)

    def store(slot, ref):
        return pltpu.make_async_copy(stage.at[slot], ref, store_sem.at[slot])

    end_rows = high - 4
    piece = largest_divisor(end_rows, 12)
    pieces = end_rows // piece

    def hand_over(k):
        rows = pl.ds(2 + k * piece, piece)
        return pltpu.make_async_remote_copy(
            src_ref=end.at[:, rows], dst_ref=end.at[:, rows],
            send_sem=pass_send.at[k], recv_sem=pass_recv.at[k],
            device_id=(1 - depth, row, col), device_id_type=MESH,
        )

    def first_layer(source, target, first_row, total, limit):
        n = largest_divisor(total, limit)

        def body(k, _):
            at = first_row + k * n
            rise = slopes(act0, 0, at, n, 0, wide)
            for c in range(halves):
                u = source[c, pl.ds(at, n)] + rise[c]
                target[c, pl.ds(at, n)] = u
                act1[c, pl.ds(at, n), 1 : 1 + wide, :] = masked_silu(u, at)
            return 0

        lax.fori_loop(0, total // n, body, 0)

    @pl.when(depth == 0)
    def _():
        x_load.wait()
        coarse_store = pltpu.make_async_copy(x, coarse_hbm.at[0], store_sem.at[2])
        coarse_store.start()
        for side in range(2):
            rows_from = 0 if side == 0 else rows_here - HALO
            cols_from = 0 if side == 0 else cols_here - HALO
            send_row[side] = (
                x[rows_from : rows_from + HALO].reshape(HALO * cols_here, channels).astype(jnp.bfloat16)
            )
            for i in range(rows_here):
                for c in range(halves):
                    flat[side, c, i * HALO : (i + 1) * HALO, :] = x[
                        i, cols_from : cols_from + HALO, c * LANES : (c + 1) * LANES
                    ]
            for c in range(halves):
                send_col[side, :, halves_of(c)] = flat[side, c].astype(jnp.bfloat16)
        peers = jnp.int32(1)
        for step in DIRECTIONS:
            exists, target = neighbour(step)
            peers = peers + jnp.where(exists, 1, 0)
        pl.semaphore_wait(barrier, peers)

        corner = HALO * HALO
        copies = []
        for k, (dr, dc) in enumerate(DIRECTIONS):
            exists, target = neighbour((dr, dc))
            if dc == 0:
                side = (dr + 1) // 2
                src, dst = send_row.at[side], recv_row.at[1 - side]
            elif dr == 0:
                side = (dc + 1) // 2
                src, dst = send_col.at[side], recv_col.at[1 - side]
            else:
                side = (dc + 1) // 2
                from_row = 0 if dr < 0 else (rows_here - HALO) * HALO
                src = send_col.at[side, pl.ds(from_row, corner)]
                dst = recv_corner.at[(1 - dr) // 2, (1 - dc) // 2]
            opposite = DIRECTIONS.index((-dr, -dc))
            copy = pltpu.make_async_remote_copy(
                src_ref=src, dst_ref=dst, send_sem=send_sem.at[k], recv_sem=recv_sem.at[opposite],
                device_id=target, device_id_type=MESH,
            )
            arrival = pltpu.make_async_remote_copy(
                src_ref=src,
                dst_ref=(
                    recv_row.at[(dr + 1) // 2] if dc == 0
                    else recv_col.at[(dc + 1) // 2] if dr == 0
                    else recv_corner.at[(dr + 1) // 2, (dc + 1) // 2]
                ),
                send_sem=send_sem.at[k], recv_sem=recv_sem.at[k],
                device_id=target, device_id_type=MESH,
            )
            copies.append((exists, copy, arrival))
        order = (4, 5, 6, 7, 2, 3, 0, 1)
        for k in order:
            exists, copy, arrival = copies[k]
            pl.when(exists)(copy.start)

        def place(i, _):
            for c in range(halves):
                base[c, i + HALO, HALO : HALO + cols_here, :] = x[i, :, halves_of(c)]
            return 0

        lax.fori_loop(0, rows_here, place, 0, unroll=4)

        for exists, copy, arrival in copies:

            @pl.when(exists)
            def _(copy=copy, arrival=arrival):
                arrival.wait_recv()

        for side in range(2):
            top = 0 if side == 0 else high - HALO
            left = 0 if side == 0 else wide - HALO
            for c in range(halves):
                base[c, top : top + HALO, HALO : HALO + cols_here, :] = (
                    recv_row[side, :, halves_of(c)].astype(jnp.float32).reshape(HALO, cols_here, LANES)
                )
                flat[side, c] = recv_col[side, :, halves_of(c)].astype(jnp.float32)
                for i in range(rows_here):
                    base[c, HALO + i, left : left + HALO, :] = flat[side, c, i * HALO : (i + 1) * HALO, :]
            for other in range(2):
                beside = 0 if other == 0 else wide - HALO
                for c in range(halves):
                    block = recv_corner[side, other, :, halves_of(c)].astype(jnp.float32)
                    for i in range(HALO):
                        base[c, top + i, beside : beside + HALO, :] = block[i * HALO : (i + 1) * HALO]

        n = largest_divisor(high, 8)

        def start_act(k, _):
            for c in range(halves):
                u = base[c, pl.ds(k * n, n)]
                act0[c, pl.ds(k * n, n), 1 : 1 + wide, :] = masked_silu(u, k * n)
            return 0

        lax.fori_loop(0, high // n, start_act, 0)
        w_loads[0].wait()
        first_layer(base, mid, 1, high - 2, 19)
        stage_interior(mid, 0)
        store(0, fine_hbm.at[0]).start()
        w_loads[1].wait()

        def second(k, _):
            at = 2 + k * piece
            rise = slopes(act1, 1, at, piece, 0, wide)
            for c in range(halves):
                end[c, pl.ds(at, piece)] = mid[c, pl.ds(at, piece)] + rise[c]
            hand_over(k).start()
            return 0

        lax.fori_loop(0, pieces, second, 0)
        stage_interior(end, 1)
        store(1, fine_hbm.at[1]).start()
        for exists, copy, arrival in copies:

            @pl.when(exists)
            def _(copy=copy):
                copy.wait_send()

        def sent(k, _):
            hand_over(k).wait_send()
            return 0

        lax.fori_loop(0, pieces, sent, 0)
        coarse_store.wait()
        store(0, fine_hbm.at[0]).wait()
        store(1, fine_hbm.at[1]).wait()

    @pl.when(depth == 1)
    def _():
        pl.semaphore_wait(barrier, 1)

        def received(k, _):
            hand_over(k).wait_recv()
            at = 2 + k * piece
            for c in range(halves):
                u = end[c, pl.ds(at, piece)]
                act0[c, pl.ds(at, piece), 1 : 1 + wide, :] = masked_silu(u, at)
            return 0

        lax.fori_loop(0, pieces, received, 0)
        stage_interior(end, 2)
        store(2, coarse_hbm.at[0]).start()
        w_loads[0].wait()
        first_layer(end, mid, 3, high - 6, 17)
        stage_interior(mid, 0)
        store(0, fine_hbm.at[0]).start()
        w_loads[1].wait()
        n = largest_divisor(rows_here, 16)

        def last(k, _):
            at = k * n
            rise = slopes(act1, 1, at + HALO, n, HALO, cols_here)
            for c in range(halves):
                stage[1, pl.ds(at, n), :, halves_of(c)] = stage[0, pl.ds(at, n), :, halves_of(c)] + rise[c]
            return 0

        lax.fori_loop(0, rows_here // n, last, 0)
        store(1, fine_hbm.at[1]).start()
        store(2, coarse_hbm.at[0]).wait()
        store(0, fine_hbm.at[0]).wait()
        store(1, fine_hbm.at[1]).wait()


def two_sections(section_states, weights):
    _, rows_here, cols_here, channels = section_states.shape
    halves = channels // LANES
    high, wide = rows_here + 2 * HALO, cols_here + 2 * HALO
    act_wide = -(-(wide + 2) // 8) * 8
    pieces = (high - 4) // largest_divisor(high - 4, 12)
    sizes = (lax.axis_size("rows"), lax.axis_size("cols"), 2.0 / (2 * lax.axis_size("depth")))
    f32, bf16, vmem = jnp.float32, jnp.bfloat16, pltpu.VMEM
    state = vmem((halves, high, wide, LANES), f32)
    act = vmem((halves, high, act_wide, LANES), f32)
    most = max(largest_divisor(high - 2, 19), largest_divisor(high - 6, 17), largest_divisor(high - 4, 12))
    most_pixels = max(most * wide, largest_divisor(rows_here, 16) * cols_here)
    flat_weights = weights.reshape(2, 9 * channels, channels)
    return pl.pallas_call(
        functools.partial(cycle_kernel, sizes),
        out_shape=(
            jax.ShapeDtypeStruct((2, rows_here, cols_here, channels), f32),
            jax.ShapeDtypeStruct((1, rows_here, cols_here, channels), f32),
        ),
        in_specs=[pl.BlockSpec(memory_space=pl.ANY)] * 2,
        out_specs=[pl.BlockSpec(memory_space=pl.ANY)] * 2,
        scratch_shapes=[
            vmem((rows_here, cols_here, channels), f32),
            vmem((2, 9 * channels, channels), bf16),
            state, state, state, act, act,
            vmem((-(-most_pixels // 16) * 16, 9 * channels), bf16),
            vmem((3, rows_here, cols_here, channels), f32),
            vmem((2, halves, rows_here * HALO, LANES), f32),
            vmem((2, HALO * cols_here, channels), bf16),
            vmem((2, rows_here * HALO, channels), bf16),
            vmem((2, HALO * cols_here, channels), bf16),
            vmem((2, rows_here * HALO, channels), bf16),
            vmem((2, 2, HALO * HALO, channels), bf16),
            pltpu.SemaphoreType.DMA((3,)),
            pltpu.SemaphoreType.DMA((3,)),
            pltpu.SemaphoreType.DMA((8,)),
            pltpu.SemaphoreType.DMA((8,)),
            pltpu.SemaphoreType.DMA((pieces,)),
            pltpu.SemaphoreType.DMA((pieces,)),
        ],
        compiler_params=pltpu.CompilerParams(collective_id=0, has_side_effects=True),
    )(section_states, flat_weights)


def on_device(section_states, weights):
    _, rows_here, cols_here, channels = section_states.shape
    tiles = rows_here % 8 == 0 and cols_here % 8 == 0 and channels % LANES == 0
    if lax.axis_size("depth") == 2 and tiles and min(rows_here, cols_here) >= HALO:
        return two_sections(section_states, weights)
    return chain_on_device(section_states, weights)


def solution(mesh):
    in_specs = (P("depth", "rows", "cols", None), P("depth", None, None, None, None))
    out_specs = (P("depth", "rows", "cols", None), P("depth", "rows", "cols", None))
    return jax.shard_map(
        on_device, mesh=mesh, in_specs=in_specs, out_specs=out_specs, check_vma=False
    )
```

```python
import functools

import jax
import jax.numpy as jnp
from jax import lax
from jax.experimental import pallas as pl
from jax.experimental.pallas import tpu as pltpu
from jax.sharding import PartitionSpec as P

MESH = pl.DeviceIdType.MESH
HALO = 4
LANES = 128
LIMIT = 32 * 1024 * 1024


def padded_2(shard, sides, width):
    for axis, dim in sides:
        size, length = (lax.axis_size(axis), shard.shape[dim])
        up = [(i, (i + 1) % size) for i in range(size - 1)]
        down = [(j, i) for i, j in up]
        last = lax.slice_in_dim(shard, length - width, length, axis=dim)
        initial = lax.slice_in_dim(shard, 0, width, axis=dim)
        before = lax.ppermute(last, axis, up)
        after = lax.ppermute(initial, axis, down)
        shard = jnp.concatenate([before, shard, after], axis=dim)
    return shard


def shifted_2(block, axis, distance):
    devices = range(lax.axis_size(axis))
    route = [(i - distance, i) for i in devices if i - distance in devices]
    return lax.ppermute(block, axis, route)


def activate(field):
    return jax.nn.silu(field).astype(jnp.bfloat16)


def apply_stencil(padded, flat_weight, out_rows, out_cols):
    channels = padded.shape[2]
    patches = jnp.concatenate(
        [
            padded[shift_row : shift_row + out_rows, shift_col : shift_col + out_cols]
            for shift_row in range(3)
            for shift_col in range(3)
        ],
        axis=2,
    )
    summed = jnp.dot(
        patches.reshape(out_rows * out_cols, 9 * channels),
        flat_weight,
        preferred_element_type=jnp.float32,
    )
    return summed.reshape(out_rows, out_cols, channels)


def section_pass(anchor, first_weight, second_weight, step_size):
    rows_here, cols_here, channels = anchor.shape
    widened = padded_2(anchor, (("rows", 0), ("cols", 1)), 2)
    slope_wide = apply_stencil(activate(widened), first_weight, rows_here + 2, cols_here + 2)
    middle_wide = widened[1:-1, 1:-1] + step_size * slope_wide
    row_global = lax.axis_index("rows") * rows_here - 1 + jnp.arange(rows_here + 2)
    col_global = lax.axis_index("cols") * cols_here - 1 + jnp.arange(cols_here + 2)
    inside_rows = (row_global >= 0) & (row_global < rows_here * lax.axis_size("rows"))
    inside_cols = (col_global >= 0) & (col_global < cols_here * lax.axis_size("cols"))
    inside = inside_rows[:, None] & inside_cols[None, :]
    second_act = jnp.where(inside[:, :, None], activate(middle_wide), jnp.zeros((), jnp.bfloat16))
    first_slope = slope_wide[1:-1, 1:-1]
    middle = middle_wide[1:-1, 1:-1]
    second_slope = apply_stencil(second_act, second_weight, rows_here, cols_here)
    ending = middle + step_size * second_slope
    return (first_slope, middle, ending)


def chain_on_device(section_states, weights):
    rows_here, cols_here, channels = section_states.shape[1:]
    ndepth = lax.axis_size("depth")
    position = lax.axis_index("depth")
    step_size = 2.0 / (2 * ndepth)
    first_weight = weights[0].reshape(9 * channels, channels)
    second_weight = weights[1].reshape(9 * channels, channels)
    anchor = section_states[0]
    first_slope, middle, ending = section_pass(anchor, first_weight, second_weight, step_size)
    jump = ending - (anchor + 2.0 * step_size * first_slope)

    def chain_turn(step_index, current):
        padded = padded_2(activate(current), (("rows", 0), ("cols", 1)), 1)
        advanced = (
            current
            + 2.0 * step_size * apply_stencil(padded, first_weight, rows_here, cols_here)
            + jump
        )
        shifted = shifted_2(advanced, "depth", 1)
        return jnp.where(position == 0, anchor, shifted)

    corrected = lax.fori_loop(0, ndepth - 1, chain_turn, anchor)
    final_slope, final_middle, final_ending = section_pass(
        corrected, first_weight, second_weight, step_size
    )
    fine_states = jnp.stack([final_middle, final_ending])
    return (fine_states, corrected[None])


def largest_divisor(total, limit):
    return max(n for n in range(1, limit + 1) if total % n == 0)


DIRECTIONS = ((-1, 0), (1, 0), (0, -1), (0, 1), (-1, -1), (-1, 1), (1, -1), (1, 1))


def cycle_kernel(
    sizes, x_hbm, w_hbm, act1, w_last, stage,
    w_first, base, mid, end, act0, patches,
    flat, send_row, send_col, recv_row, recv_col, recv_corner,
    load_sem, send_sem, recv_sem, pass_send, pass_recv,
):
    nrows, ncols, step_size = sizes
    x = stage.at[2]
    w = (w_first, w_last)
    rows_here, cols_here, channels = x.shape
    halves = channels // LANES
    high, wide = rows_here + 2 * HALO, cols_here + 2 * HALO
    depth, row, col = lax.axis_index("depth"), lax.axis_index("rows"), lax.axis_index("cols")

    x_load = pltpu.make_async_copy(x_hbm.at[0], x, load_sem.at[0])
    w_loads = [pltpu.make_async_copy(w_hbm.at[k], w[k], load_sem.at[1 + k]) for k in range(2)]

    barrier = pltpu.get_barrier_semaphore()

    def neighbour(step):
        there_row, there_col = row + step[0], col + step[1]
        exists = (there_row >= 0) & (there_row < nrows) & (there_col >= 0) & (there_col < ncols)
        return exists, (depth, there_row, there_col)

    @pl.when(depth == 0)
    def _():
        x_load.start()

    for copy in w_loads:
        copy.start()
    pl.semaphore_signal(barrier, inc=1, device_id=(1 - depth, row, col), device_id_type=MESH)

    @pl.when(depth == 0)
    def _():
        for step in DIRECTIONS:
            exists, target = neighbour(step)

            @pl.when(exists)
            def _():
                pl.semaphore_signal(barrier, inc=1, device_id=target, device_id_type=MESH)

    def halves_of(c):
        return pl.ds(c * LANES, LANES)

    def masked_silu(u, first_row):
        n = u.shape[0]
        i = first_row + lax.broadcasted_iota(jnp.int32, (n, wide, LANES), 0) + (row * rows_here - HALO)
        j = lax.broadcasted_iota(jnp.int32, (n, wide, LANES), 1) + (col * cols_here - HALO)
        inside = (i >= 0) & (i < nrows * rows_here) & (j >= 0) & (j < ncols * cols_here)
        return jnp.where(inside, u / (1.0 + jnp.exp(-u)), 0.0)

    def slopes(act, layer, first_row, n, left, width):
        m = n * width
        for a in range(3):
            for b in range(3):
                for c in range(halves):
                    window = act[c, pl.ds(first_row + a - 1, n), left + b : left + b + width, :]
                    patches[0:m, pl.ds((a * 3 + b) * channels + c * LANES, LANES)] = (
                        window.reshape(m, LANES).astype(jnp.bfloat16)
                    )
        acc = jnp.dot(patches[0:m, :], w[layer][...], preferred_element_type=jnp.float32)
        return [
            step_size * acc[:, c * LANES : (c + 1) * LANES].reshape(n, width, LANES)
            for c in range(halves)
        ]

    def stage_interior(state, slot):
        def body(i, _):
            for c in range(halves):
                stage[slot, i, :, halves_of(c)] = state[c, i + HALO, HALO : HALO + cols_here, :]
            return 0

        lax.fori_loop(0, rows_here, body, 0, unroll=4)

    end_rows = high - 4
    piece = largest_divisor(end_rows, 12)
    pieces = end_rows // piece

    def hand_over(k):
        rows = pl.ds(2 + k * piece, piece)
        return pltpu.make_async_remote_copy(
            src_ref=end.at[:, rows], dst_ref=end.at[:, rows],
            send_sem=pass_send.at[k], recv_sem=pass_recv.at[k],
            device_id=(1 - depth, row, col), device_id_type=MESH,
        )

    def first_layer(source, target, first_row, total, limit):
        n = largest_divisor(total, limit)

        def body(k, _):
            at = first_row + k * n
            rise = slopes(act0, 0, at, n, 0, wide)
            for c in range(halves):
                u = source[c, pl.ds(at, n)] + rise[c]
                target[c, pl.ds(at, n)] = u
                act1[c, pl.ds(at, n), 1 : 1 + wide, :] = masked_silu(u, at)
            return 0

        lax.fori_loop(0, total // n, body, 0)

    @pl.when(depth == 0)
    def _():
        x_load.wait()
        for side in range(2):
            rows_from = 0 if side == 0 else rows_here - HALO
            cols_from = 0 if side == 0 else cols_here - HALO
            send_row[side] = (
                x[rows_from : rows_from + HALO].reshape(HALO * cols_here, channels).astype(jnp.bfloat16)
            )
            for i in range(rows_here):
                for c in range(halves):
                    flat[side, c, i * HALO : (i + 1) * HALO, :] = x[
                        i, cols_from : cols_from + HALO, c * LANES : (c + 1) * LANES
                    ]
            for c in range(halves):
                send_col[side, :, halves_of(c)] = flat[side, c].astype(jnp.bfloat16)
        peers = jnp.int32(1)
        for step in DIRECTIONS:
            exists, target = neighbour(step)
            peers = peers + jnp.where(exists, 1, 0)
        pl.semaphore_wait(barrier, peers)

        corner = HALO * HALO
        copies = []
        for k, (dr, dc) in enumerate(DIRECTIONS):
            exists, target = neighbour((dr, dc))
            if dc == 0:
                side = (dr + 1) // 2
                src, dst = send_row.at[side], recv_row.at[1 - side]
            elif dr == 0:
                side = (dc + 1) // 2
                src, dst = send_col.at[side], recv_col.at[1 - side]
            else:
                side = (dc + 1) // 2
                from_row = 0 if dr < 0 else (rows_here - HALO) * HALO
                src = send_col.at[side, pl.ds(from_row, corner)]
                dst = recv_corner.at[(1 - dr) // 2, (1 - dc) // 2]
            opposite = DIRECTIONS.index((-dr, -dc))
            copy = pltpu.make_async_remote_copy(
                src_ref=src, dst_ref=dst, send_sem=send_sem.at[k], recv_sem=recv_sem.at[opposite],
                device_id=target, device_id_type=MESH,
            )
            arrival = pltpu.make_async_remote_copy(
                src_ref=src,
                dst_ref=(
                    recv_row.at[(dr + 1) // 2] if dc == 0
                    else recv_col.at[(dc + 1) // 2] if dr == 0
                    else recv_corner.at[(dr + 1) // 2, (dc + 1) // 2]
                ),
                send_sem=send_sem.at[k], recv_sem=recv_sem.at[k],
                device_id=target, device_id_type=MESH,
            )
            copies.append((exists, copy, arrival))
        order = (4, 5, 6, 7, 2, 3, 0, 1)
        for k in order:
            exists, copy, arrival = copies[k]
            pl.when(exists)(copy.start)

        def place(i, _):
            for c in range(halves):
                base[c, i + HALO, HALO : HALO + cols_here, :] = x[i, :, halves_of(c)]
            return 0

        lax.fori_loop(0, rows_here, place, 0, unroll=4)

        for exists, copy, arrival in copies:

            @pl.when(exists)
            def _(copy=copy, arrival=arrival):
                arrival.wait_recv()

        for side in range(2):
            top = 0 if side == 0 else high - HALO
            left = 0 if side == 0 else wide - HALO
            for c in range(halves):
                base[c, top : top + HALO, HALO : HALO + cols_here, :] = (
                    recv_row[side, :, halves_of(c)].astype(jnp.float32).reshape(HALO, cols_here, LANES)
                )
                flat[side, c] = recv_col[side, :, halves_of(c)].astype(jnp.float32)
                for i in range(rows_here):
                    base[c, HALO + i, left : left + HALO, :] = flat[side, c, i * HALO : (i + 1) * HALO, :]
            for other in range(2):
                beside = 0 if other == 0 else wide - HALO
                for c in range(halves):
                    block = recv_corner[side, other, :, halves_of(c)].astype(jnp.float32)
                    for i in range(HALO):
                        base[c, top + i, beside : beside + HALO, :] = block[i * HALO : (i + 1) * HALO]

        n = largest_divisor(high, 8)

        def start_act(k, _):
            for c in range(halves):
                u = base[c, pl.ds(k * n, n)]
                act0[c, pl.ds(k * n, n), 1 : 1 + wide, :] = masked_silu(u, k * n)
            return 0

        lax.fori_loop(0, high // n, start_act, 0)
        w_loads[0].wait()
        first_layer(base, mid, 1, high - 2, 19)
        stage_interior(mid, 0)
        w_loads[1].wait()

        def second(k, _):
            at = 2 + k * piece
            rise = slopes(act1, 1, at, piece, 0, wide)
            for c in range(halves):
                end[c, pl.ds(at, piece)] = mid[c, pl.ds(at, piece)] + rise[c]
            hand_over(k).start()
            return 0

        lax.fori_loop(0, pieces, second, 0)
        stage_interior(end, 1)
        for exists, copy, arrival in copies:

            @pl.when(exists)
            def _(copy=copy):
                copy.wait_send()

        def sent(k, _):
            hand_over(k).wait_send()
            return 0

        lax.fori_loop(0, pieces, sent, 0)

    @pl.when(depth == 1)
    def _():
        pl.semaphore_wait(barrier, 1)

        def received(k, _):
            hand_over(k).wait_recv()
            at = 2 + k * piece
            for c in range(halves):
                u = end[c, pl.ds(at, piece)]
                act0[c, pl.ds(at, piece), 1 : 1 + wide, :] = masked_silu(u, at)
            return 0

        lax.fori_loop(0, pieces, received, 0)
        stage_interior(end, 2)
        w_loads[0].wait()
        first_layer(end, mid, 3, high - 6, 17)
        stage_interior(mid, 0)
        w_loads[1].wait()


def last_kernel(
    step_size, act, w, stage, fine_hbm, coarse_hbm, patches, ending, store_sem, piece_sem
):
    _, rows_here, cols_here, channels = stage.shape
    halves = channels // LANES
    depth = lax.axis_index("depth")
    pieces = piece_sem.shape[0]
    n = rows_here // pieces
    m = n * cols_here

    def store(slot, ref):
        return pltpu.make_async_copy(stage.at[slot], ref, store_sem.at[slot])

    coarse_store = store(2, coarse_hbm.at[0])
    first_store = store(0, fine_hbm.at[0])
    coarse_store.start()
    first_store.start()

    @pl.when(depth == 0)
    def _():
        second_store = store(1, fine_hbm.at[1])
        second_store.start()
        second_store.wait()

    @pl.when(depth == 1)
    def _():
        def piece_store(k):
            rows = pl.ds(k * n, n)
            return pltpu.make_async_copy(ending.at[rows], fine_hbm.at[1, rows], piece_sem.at[k])

        def last(k, _):
            at = k * n
            for a in range(3):
                for b in range(3):
                    for c in range(halves):
                        window = act[c, pl.ds(at + HALO + a - 1, n), HALO + b : HALO + b + cols_here, :]
                        patches[:, pl.ds((a * 3 + b) * channels + c * LANES, LANES)] = (
                            window.reshape(m, LANES).astype(jnp.bfloat16)
                        )
            acc = jnp.dot(patches[...], w[...], preferred_element_type=jnp.float32)
            ending[pl.ds(at, n)] = stage[0, pl.ds(at, n)] + step_size * acc.reshape(n, cols_here, channels)
            piece_store(k).start()
            return 0

        lax.fori_loop(0, pieces, last, 0)
        for k in range(pieces):
            piece_store(k).wait()

    coarse_store.wait()
    first_store.wait()


def two_sections(section_states, weights):
    _, rows_here, cols_here, channels = section_states.shape
    halves = channels // LANES
    high, wide = rows_here + 2 * HALO, cols_here + 2 * HALO
    act_wide = -(-(wide + 2) // 8) * 8
    pieces = (high - 4) // largest_divisor(high - 4, 12)
    sizes = (lax.axis_size("rows"), lax.axis_size("cols"), 2.0 / (2 * lax.axis_size("depth")))
    f32, bf16, vmem = jnp.float32, jnp.bfloat16, pltpu.VMEM
    state = vmem((halves, high, wide, LANES), f32)
    act = vmem((halves, high, act_wide, LANES), f32)
    most = max(largest_divisor(high - 2, 19), largest_divisor(high - 6, 17), largest_divisor(high - 4, 12))
    most_pixels = max(most * wide, largest_divisor(rows_here, 16) * cols_here)
    flat_weights = weights.reshape(2, 9 * channels, channels)
    any_space, in_vmem = pl.BlockSpec(memory_space=pl.ANY), pl.BlockSpec(memory_space=vmem)
    act_last, w_last, stage = pl.pallas_call(
        functools.partial(cycle_kernel, sizes),
        out_shape=(
            act,
            vmem((9 * channels, channels), bf16),
            vmem((3, rows_here, cols_here, channels), f32),
        ),
        in_specs=[pl.BlockSpec(memory_space=pltpu.HBM)] * 2,
        out_specs=[in_vmem] * 3,
        scratch_shapes=[
            vmem((9 * channels, channels), bf16),
            state, state, state, act,
            vmem((-(-most_pixels // 16) * 16, 9 * channels), bf16),
            vmem((2, halves, rows_here * HALO, LANES), f32),
            vmem((2, HALO * cols_here, channels), bf16),
            vmem((2, rows_here * HALO, channels), bf16),
            vmem((2, HALO * cols_here, channels), bf16),
            vmem((2, rows_here * HALO, channels), bf16),
            vmem((2, 2, HALO * HALO, channels), bf16),
            pltpu.SemaphoreType.DMA((3,)),
            pltpu.SemaphoreType.DMA((8,)),
            pltpu.SemaphoreType.DMA((8,)),
            pltpu.SemaphoreType.DMA((pieces,)),
            pltpu.SemaphoreType.DMA((pieces,)),
        ],
        compiler_params=pltpu.CompilerParams(
            collective_id=0, has_side_effects=True, vmem_limit_bytes=LIMIT
        ),
    )(
        pltpu.with_memory_space_constraint(section_states, pltpu.HBM),
        pltpu.with_memory_space_constraint(flat_weights, pltpu.HBM),
    )
    last_pieces = rows_here // largest_divisor(rows_here, 8)
    return pl.pallas_call(
        functools.partial(last_kernel, sizes[2]),
        out_shape=(
            jax.ShapeDtypeStruct((2, rows_here, cols_here, channels), f32),
            jax.ShapeDtypeStruct((1, rows_here, cols_here, channels), f32),
        ),
        in_specs=[in_vmem] * 3,
        out_specs=[any_space] * 2,
        scratch_shapes=[
            vmem((rows_here // last_pieces * cols_here, 9 * channels), bf16),
            vmem((rows_here, cols_here, channels), f32),
            pltpu.SemaphoreType.DMA((3,)),
            pltpu.SemaphoreType.DMA((last_pieces,)),
        ],
        compiler_params=pltpu.CompilerParams(vmem_limit_bytes=LIMIT),
    )(act_last, w_last, stage)


def on_device(section_states, weights):
    _, rows_here, cols_here, channels = section_states.shape
    tiles = rows_here % 8 == 0 and cols_here % 8 == 0 and channels % LANES == 0
    if lax.axis_size("depth") == 2 and tiles and min(rows_here, cols_here) >= HALO:
        return two_sections(section_states, weights)
    return chain_on_device(section_states, weights)


def solution(mesh):
    in_specs = (P("depth", "rows", "cols", None), P("depth", None, None, None, None))
    out_specs = (P("depth", "rows", "cols", None), P("depth", "rows", "cols", None))
    return jax.shard_map(
        on_device, mesh=mesh, in_specs=in_specs, out_specs=out_specs, check_vma=False
    )
```

```python
import functools

import jax
import jax.numpy as jnp
from jax import lax
from jax.experimental import pallas as pl
from jax.experimental.pallas import tpu as pltpu
from jax.sharding import PartitionSpec as P

MESH = pl.DeviceIdType.MESH
HALO = 4
LANES = 128
LIMIT = 32 * 1024 * 1024


def padded_2(shard, sides, width):
    for axis, dim in sides:
        size, length = (lax.axis_size(axis), shard.shape[dim])
        up = [(i, (i + 1) % size) for i in range(size - 1)]
        down = [(j, i) for i, j in up]
        last = lax.slice_in_dim(shard, length - width, length, axis=dim)
        initial = lax.slice_in_dim(shard, 0, width, axis=dim)
        before = lax.ppermute(last, axis, up)
        after = lax.ppermute(initial, axis, down)
        shard = jnp.concatenate([before, shard, after], axis=dim)
    return shard


def shifted_2(block, axis, distance):
    devices = range(lax.axis_size(axis))
    route = [(i - distance, i) for i in devices if i - distance in devices]
    return lax.ppermute(block, axis, route)


def activate(field):
    return jax.nn.silu(field).astype(jnp.bfloat16)


def apply_stencil(padded, flat_weight, out_rows, out_cols):
    channels = padded.shape[2]
    patches = jnp.concatenate(
        [
            padded[shift_row : shift_row + out_rows, shift_col : shift_col + out_cols]
            for shift_row in range(3)
            for shift_col in range(3)
        ],
        axis=2,
    )
    summed = jnp.dot(
        patches.reshape(out_rows * out_cols, 9 * channels),
        flat_weight,
        preferred_element_type=jnp.float32,
    )
    return summed.reshape(out_rows, out_cols, channels)


def section_pass(anchor, first_weight, second_weight, step_size):
    rows_here, cols_here, channels = anchor.shape
    widened = padded_2(anchor, (("rows", 0), ("cols", 1)), 2)
    slope_wide = apply_stencil(activate(widened), first_weight, rows_here + 2, cols_here + 2)
    middle_wide = widened[1:-1, 1:-1] + step_size * slope_wide
    row_global = lax.axis_index("rows") * rows_here - 1 + jnp.arange(rows_here + 2)
    col_global = lax.axis_index("cols") * cols_here - 1 + jnp.arange(cols_here + 2)
    inside_rows = (row_global >= 0) & (row_global < rows_here * lax.axis_size("rows"))
    inside_cols = (col_global >= 0) & (col_global < cols_here * lax.axis_size("cols"))
    inside = inside_rows[:, None] & inside_cols[None, :]
    second_act = jnp.where(inside[:, :, None], activate(middle_wide), jnp.zeros((), jnp.bfloat16))
    first_slope = slope_wide[1:-1, 1:-1]
    middle = middle_wide[1:-1, 1:-1]
    second_slope = apply_stencil(second_act, second_weight, rows_here, cols_here)
    ending = middle + step_size * second_slope
    return (first_slope, middle, ending)


def chain_on_device(section_states, weights):
    rows_here, cols_here, channels = section_states.shape[1:]
    ndepth = lax.axis_size("depth")
    position = lax.axis_index("depth")
    step_size = 2.0 / (2 * ndepth)
    first_weight = weights[0].reshape(9 * channels, channels)
    second_weight = weights[1].reshape(9 * channels, channels)
    anchor = section_states[0]
    first_slope, middle, ending = section_pass(anchor, first_weight, second_weight, step_size)
    jump = ending - (anchor + 2.0 * step_size * first_slope)

    def chain_turn(step_index, current):
        padded = padded_2(activate(current), (("rows", 0), ("cols", 1)), 1)
        advanced = (
            current
            + 2.0 * step_size * apply_stencil(padded, first_weight, rows_here, cols_here)
            + jump
        )
        shifted = shifted_2(advanced, "depth", 1)
        return jnp.where(position == 0, anchor, shifted)

    corrected = lax.fori_loop(0, ndepth - 1, chain_turn, anchor)
    final_slope, final_middle, final_ending = section_pass(
        corrected, first_weight, second_weight, step_size
    )
    fine_states = jnp.stack([final_middle, final_ending])
    return (fine_states, corrected[None])


def largest_divisor(total, limit):
    return max(n for n in range(1, limit + 1) if total % n == 0)


DIRECTIONS = ((-1, 0), (1, 0), (0, -1), (0, 1), (-1, -1), (-1, 1), (1, -1), (1, 1))


def cycle_kernel(
    sizes, x_hbm, w_hbm, act1, w_last, stage,
    w_first, base, mid, end, act0, inside, patches,
    flat, send_row, send_col, recv_row, recv_col, recv_corner,
    load_sem, send_sem, recv_sem, pass_send, pass_recv,
):
    nrows, ncols, step_size = sizes
    x = stage.at[2]
    w = (w_first, w_last)
    rows_here, cols_here, channels = x.shape
    halves = channels // LANES
    high, wide = rows_here + 2 * HALO, cols_here + 2 * HALO
    depth, row, col = lax.axis_index("depth"), lax.axis_index("rows"), lax.axis_index("cols")

    x_load = pltpu.make_async_copy(x_hbm.at[0], x, load_sem.at[0])
    w_loads = [pltpu.make_async_copy(w_hbm.at[k], w[k], load_sem.at[1 + k]) for k in range(2)]

    barrier = pltpu.get_barrier_semaphore()

    def neighbour(step):
        there_row, there_col = row + step[0], col + step[1]
        exists = (there_row >= 0) & (there_row < nrows) & (there_col >= 0) & (there_col < ncols)
        return exists, (depth, there_row, there_col)

    @pl.when(depth == 0)
    def _():
        x_load.start()

    for copy in w_loads:
        copy.start()
    pl.semaphore_signal(barrier, inc=1, device_id=(1 - depth, row, col), device_id_type=MESH)

    @pl.when(depth == 0)
    def _():
        for step in DIRECTIONS:
            exists, target = neighbour(step)

            @pl.when(exists)
            def _():
                pl.semaphore_signal(barrier, inc=1, device_id=target, device_id_type=MESH)

    def halves_of(c):
        return pl.ds(c * LANES, LANES)

    def silu(u):
        half = 0.5 * u
        return half + half * jnp.tanh(half)

    def masked_silu(u, first_row):
        half = 0.5 * u
        kept = half * inside[pl.ds(first_row, u.shape[0])]
        return kept + kept * jnp.tanh(half)

    def mark_inside(k, _):
        i = lax.broadcasted_iota(jnp.int32, (1, wide, LANES), 0) + (row * rows_here - HALO + k)
        j = lax.broadcasted_iota(jnp.int32, (1, wide, LANES), 1) + (col * cols_here - HALO)
        held = (i >= 0) & (i < nrows * rows_here) & (j >= 0) & (j < ncols * cols_here)
        inside[pl.ds(k, 1)] = jnp.where(held, 1.0, 0.0)
        return 0

    lax.fori_loop(0, high, mark_inside, 0, unroll=4)

    def slopes(act, layer, first_row, n, slot):
        m, width, left = n * wide, wide, 0
        for a in range(3):
            for b in range(3):
                for c in range(halves):
                    window = act[c, pl.ds(first_row + a - 1, n), left + b : left + b + width, :]
                    patches[slot, 0:m, pl.ds((a * 3 + b) * channels + c * LANES, LANES)] = (
                        window.reshape(m, LANES).astype(jnp.bfloat16)
                    )
        acc = jnp.dot(patches[slot, 0:m, :], w[layer][...], preferred_element_type=jnp.float32)
        return [
            step_size * acc[:, c * LANES : (c + 1) * LANES].reshape(n, width, LANES)
            for c in range(halves)
        ]

    def stage_interior(state, slot):
        def body(i, _):
            for c in range(halves):
                stage[slot, i, :, halves_of(c)] = state[c, i + HALO, HALO : HALO + cols_here, :]
            return 0

        lax.fori_loop(0, rows_here, body, 0, unroll=4)

    end_rows = high - 4
    piece = largest_divisor(end_rows, 9)
    pieces = end_rows // piece

    def hand_over(k):
        rows = pl.ds(2 + k * piece, piece)
        return pltpu.make_async_remote_copy(
            src_ref=end.at[:, rows], dst_ref=end.at[:, rows],
            send_sem=pass_send.at[k], recv_sem=pass_recv.at[k],
            device_id=(1 - depth, row, col), device_id_type=MESH,
        )

    def first_layer(source, target, first_row, total, limit, unrolled):
        n = largest_divisor(total, limit)

        def body(k, _):
            at = first_row + k * n
            rise = slopes(act0, 0, at, n, k % 2 if unrolled else 0)
            for c in range(halves):
                u = source[c, pl.ds(at, n)] + rise[c]
                target[c, pl.ds(at, n)] = u
                act1[c, pl.ds(at, n), 1 : 1 + wide, :] = masked_silu(u, at)
            return 0

        if unrolled:
            for k in range(total // n):
                body(k, 0)
        else:
            lax.fori_loop(0, total // n, body, 0)

    @pl.when(depth == 0)
    def _():
        def clear(i, _):
            for c in range(halves):
                base[c, pl.ds(i, 1)] = jnp.zeros((1, wide, LANES), jnp.float32)
                act0[c, pl.ds(i, 1)] = jnp.zeros((1,) + act0.shape[2:], jnp.float32)
            return 0

        lax.fori_loop(0, high, clear, 0, unroll=4)
        x_load.wait()
        for side in range(2):
            rows_from = 0 if side == 0 else rows_here - HALO
            cols_from = 0 if side == 0 else cols_here - HALO
            send_row[side] = (
                x[rows_from : rows_from + HALO].reshape(HALO * cols_here, channels).astype(jnp.bfloat16)
            )
            for i in range(rows_here):
                for c in range(halves):
                    flat[side, c, i * HALO : (i + 1) * HALO, :] = x[
                        i, cols_from : cols_from + HALO, c * LANES : (c + 1) * LANES
                    ]
            for c in range(halves):
                send_col[side, :, halves_of(c)] = flat[side, c].astype(jnp.bfloat16)
        peers = jnp.int32(1)
        for step in DIRECTIONS:
            exists, target = neighbour(step)
            peers = peers + jnp.where(exists, 1, 0)
        pl.semaphore_wait(barrier, peers)

        corner = HALO * HALO
        copies = []
        for k, (dr, dc) in enumerate(DIRECTIONS):
            exists, target = neighbour((dr, dc))
            if dc == 0:
                side = (dr + 1) // 2
                src, dst = send_row.at[side], recv_row.at[1 - side]
            elif dr == 0:
                side = (dc + 1) // 2
                src, dst = send_col.at[side], recv_col.at[1 - side]
            else:
                side = (dc + 1) // 2
                from_row = 0 if dr < 0 else (rows_here - HALO) * HALO
                src = send_col.at[side, pl.ds(from_row, corner)]
                dst = recv_corner.at[(1 - dr) // 2, (1 - dc) // 2]
            opposite = DIRECTIONS.index((-dr, -dc))
            copy = pltpu.make_async_remote_copy(
                src_ref=src, dst_ref=dst, send_sem=send_sem.at[k], recv_sem=recv_sem.at[opposite],
                device_id=target, device_id_type=MESH,
            )
            arrival = pltpu.make_async_remote_copy(
                src_ref=src,
                dst_ref=(
                    recv_row.at[(dr + 1) // 2] if dc == 0
                    else recv_col.at[(dc + 1) // 2] if dr == 0
                    else recv_corner.at[(dr + 1) // 2, (dc + 1) // 2]
                ),
                send_sem=send_sem.at[k], recv_sem=recv_sem.at[k],
                device_id=target, device_id_type=MESH,
            )
            copies.append((exists, copy, arrival))
        order = (4, 5, 6, 7, 2, 3, 0, 1)
        for k in order:
            exists, copy, arrival = copies[k]
            pl.when(exists)(copy.start)

        def place(i, _):
            for c in range(halves):
                u = x[i, :, halves_of(c)]
                base[c, i + HALO, HALO : HALO + cols_here, :] = u
                act0[c, i + HALO, HALO + 1 : HALO + 1 + cols_here, :] = silu(u)
            return 0

        lax.fori_loop(0, rows_here, place, 0, unroll=4)

        def put(c, i, j, u, act):
            base[c, i, j : j + u.shape[0], :] = u
            act0[c, i, j + 1 : j + 1 + u.shape[0], :] = act

        for k in (2, 3, 0, 1, 4, 5, 6, 7):
            exists, copy, arrival = copies[k]
            dr, dc = DIRECTIONS[k]

            @pl.when(exists)
            def _(arrival=arrival, dr=dr, dc=dc):
                arrival.wait_recv()
                top = {-1: 0, 0: HALO, 1: high - HALO}[dr]
                left = {-1: 0, 0: HALO, 1: wide - HALO}[dc]
                for c in range(halves):
                    if dr == 0:
                        side = (dc + 1) // 2
                        u = recv_col[side, :, halves_of(c)].astype(jnp.float32)
                        flat[0, c] = u
                        flat[1, c] = silu(u)
                        for i in range(rows_here):
                            part = slice(i * HALO, (i + 1) * HALO)
                            put(c, top + i, left, flat[0, c, part, :], flat[1, c, part, :])
                        continue
                    if dc == 0:
                        u = recv_row[(dr + 1) // 2, :, halves_of(c)].astype(jnp.float32)
                    else:
                        u = recv_corner[(dr + 1) // 2, (dc + 1) // 2, :, halves_of(c)].astype(jnp.float32)
                    act, n = silu(u), u.shape[0] // HALO
                    for i in range(HALO):
                        part = slice(i * n, (i + 1) * n)
                        put(c, top + i, left, u[part], act[part])

        w_loads[0].wait()
        first_layer(base, mid, 1, high - 2, 19, False)
        stage_interior(mid, 0)
        w_loads[1].wait()

        def second(k, _):
            at = 2 + k * piece
            rise = slopes(act1, 1, at, piece, 0)
            for c in range(halves):
                end[c, pl.ds(at, piece)] = mid[c, pl.ds(at, piece)] + rise[c]
            hand_over(k).start()
            return 0

        lax.fori_loop(0, pieces, second, 0)
        stage_interior(end, 1)
        for exists, copy, arrival in copies:

            @pl.when(exists)
            def _(copy=copy):
                copy.wait_send()

        def sent(k, _):
            hand_over(k).wait_send()
            return 0

        lax.fori_loop(0, pieces, sent, 0)

    @pl.when(depth == 1)
    def _():
        pl.semaphore_wait(barrier, 1)

        def received(k, _):
            hand_over(k).wait_recv()
            at = 2 + k * piece
            for c in range(halves):
                u = end[c, pl.ds(at, piece)]
                act0[c, pl.ds(at, piece), 1 : 1 + wide, :] = masked_silu(u, at)
            return 0

        lax.fori_loop(0, pieces, received, 0)
        stage_interior(end, 2)
        w_loads[0].wait()
        first_layer(end, mid, 3, high - 6, 17, True)
        stage_interior(mid, 0)
        w_loads[1].wait()


def last_kernel(
    step_size, act, w, stage, fine_hbm, coarse_hbm, patches, ending, store_sem, piece_sem
):
    _, rows_here, cols_here, channels = stage.shape
    halves = channels // LANES
    depth = lax.axis_index("depth")
    pieces = piece_sem.shape[0]
    n = rows_here // pieces
    m = n * cols_here

    def store(slot, ref):
        return pltpu.make_async_copy(stage.at[slot], ref, store_sem.at[slot])

    coarse_store = store(2, coarse_hbm.at[0])
    first_store = store(0, fine_hbm.at[0])
    coarse_store.start()
    first_store.start()

    @pl.when(depth == 0)
    def _():
        second_store = store(1, fine_hbm.at[1])
        second_store.start()
        second_store.wait()

    @pl.when(depth == 1)
    def _():
        def piece_store(k):
            rows = pl.ds(k * n, n)
            return pltpu.make_async_copy(ending.at[rows], fine_hbm.at[1, rows], piece_sem.at[k])

        def last(k):
            at = k * n
            for a in range(3):
                for b in range(3):
                    for c in range(halves):
                        window = act[c, pl.ds(at + HALO + a - 1, n), HALO + b : HALO + b + cols_here, :]
                        patches[k % 2, :, pl.ds((a * 3 + b) * channels + c * LANES, LANES)] = (
                            window.reshape(m, LANES).astype(jnp.bfloat16)
                        )
            acc = jnp.dot(patches[k % 2], w[...], preferred_element_type=jnp.float32)
            ending[pl.ds(at, n)] = stage[0, pl.ds(at, n)] + step_size * acc.reshape(n, cols_here, channels)
            piece_store(k).start()

        for k in range(pieces):
            last(k)
        for k in range(pieces):
            piece_store(k).wait()

    coarse_store.wait()
    first_store.wait()


def two_sections(section_states, weights):
    _, rows_here, cols_here, channels = section_states.shape
    halves = channels // LANES
    high, wide = rows_here + 2 * HALO, cols_here + 2 * HALO
    act_wide = -(-(wide + 2) // 8) * 8
    pieces = (high - 4) // largest_divisor(high - 4, 9)
    sizes = (lax.axis_size("rows"), lax.axis_size("cols"), 2.0 / (2 * lax.axis_size("depth")))
    f32, bf16, vmem = jnp.float32, jnp.bfloat16, pltpu.VMEM
    state = vmem((halves, high, wide, LANES), f32)
    act = vmem((halves, high, act_wide, LANES), f32)
    most = max(largest_divisor(high - 2, 19), largest_divisor(high - 6, 17), largest_divisor(high - 4, 9))
    most_pixels = most * wide
    flat_weights = weights.reshape(2, 9 * channels, channels)
    any_space, in_vmem = pl.BlockSpec(memory_space=pl.ANY), pl.BlockSpec(memory_space=vmem)
    act_last, w_last, stage = pl.pallas_call(
        functools.partial(cycle_kernel, sizes),
        out_shape=(
            act,
            vmem((9 * channels, channels), bf16),
            vmem((3, rows_here, cols_here, channels), f32),
        ),
        in_specs=[pl.BlockSpec(memory_space=pltpu.HBM)] * 2,
        out_specs=[in_vmem] * 3,
        scratch_shapes=[
            vmem((9 * channels, channels), bf16),
            state, state, state, act,
            vmem((high, wide, LANES), f32),
            vmem((2, -(-most_pixels // 16) * 16, 9 * channels), bf16),
            vmem((2, halves, rows_here * HALO, LANES), f32),
            vmem((2, HALO * cols_here, channels), bf16),
            vmem((2, rows_here * HALO, channels), bf16),
            vmem((2, HALO * cols_here, channels), bf16),
            vmem((2, rows_here * HALO, channels), bf16),
            vmem((2, 2, HALO * HALO, channels), bf16),
            pltpu.SemaphoreType.DMA((3,)),
            pltpu.SemaphoreType.DMA((8,)),
            pltpu.SemaphoreType.DMA((8,)),
            pltpu.SemaphoreType.DMA((pieces,)),
            pltpu.SemaphoreType.DMA((pieces,)),
        ],
        compiler_params=pltpu.CompilerParams(
            collective_id=0, has_side_effects=True, vmem_limit_bytes=LIMIT
        ),
    )(
        pltpu.with_memory_space_constraint(section_states, pltpu.HBM),
        pltpu.with_memory_space_constraint(flat_weights, pltpu.HBM),
    )
    last_pieces = rows_here // largest_divisor(rows_here, 8)
    return pl.pallas_call(
        functools.partial(last_kernel, sizes[2]),
        out_shape=(
            jax.ShapeDtypeStruct((2, rows_here, cols_here, channels), f32),
            jax.ShapeDtypeStruct((1, rows_here, cols_here, channels), f32),
        ),
        in_specs=[in_vmem] * 3,
        out_specs=[any_space] * 2,
        scratch_shapes=[
            vmem((2, rows_here // last_pieces * cols_here, 9 * channels), bf16),
            vmem((rows_here, cols_here, channels), f32),
            pltpu.SemaphoreType.DMA((3,)),
            pltpu.SemaphoreType.DMA((last_pieces,)),
        ],
        compiler_params=pltpu.CompilerParams(vmem_limit_bytes=LIMIT),
    )(act_last, w_last, stage)


def on_device(section_states, weights):
    _, rows_here, cols_here, channels = section_states.shape
    tiles = rows_here % 8 == 0 and cols_here % 8 == 0 and channels % LANES == 0
    if lax.axis_size("depth") == 2 and tiles and min(rows_here, cols_here) >= HALO:
        return two_sections(section_states, weights)
    return chain_on_device(section_states, weights)


def solution(mesh):
    in_specs = (P("depth", "rows", "cols", None), P("depth", None, None, None, None))
    out_specs = (P("depth", "rows", "cols", None), P("depth", "rows", "cols", None))
    return jax.shard_map(
        on_device, mesh=mesh, in_specs=in_specs, out_specs=out_specs, check_vma=False
    )
```

```python
import functools

import jax
import jax.numpy as jnp
from jax import lax
from jax.experimental import pallas as pl
from jax.experimental.pallas import tpu as pltpu
from jax.sharding import PartitionSpec as P

MESH = pl.DeviceIdType.MESH
HALO = 4
LANES = 128
LIMIT = 32 * 1024 * 1024


def padded_2(shard, sides, width):
    for axis, dim in sides:
        size, length = (lax.axis_size(axis), shard.shape[dim])
        up = [(i, (i + 1) % size) for i in range(size - 1)]
        down = [(j, i) for i, j in up]
        last = lax.slice_in_dim(shard, length - width, length, axis=dim)
        initial = lax.slice_in_dim(shard, 0, width, axis=dim)
        before = lax.ppermute(last, axis, up)
        after = lax.ppermute(initial, axis, down)
        shard = jnp.concatenate([before, shard, after], axis=dim)
    return shard


def shifted_2(block, axis, distance):
    devices = range(lax.axis_size(axis))
    route = [(i - distance, i) for i in devices if i - distance in devices]
    return lax.ppermute(block, axis, route)


def activate(field):
    return jax.nn.silu(field).astype(jnp.bfloat16)


def apply_stencil(padded, flat_weight, out_rows, out_cols):
    channels = padded.shape[2]
    patches = jnp.concatenate(
        [
            padded[shift_row : shift_row + out_rows, shift_col : shift_col + out_cols]
            for shift_row in range(3)
            for shift_col in range(3)
        ],
        axis=2,
    )
    summed = jnp.dot(
        patches.reshape(out_rows * out_cols, 9 * channels),
        flat_weight,
        preferred_element_type=jnp.float32,
    )
    return summed.reshape(out_rows, out_cols, channels)


def section_pass(anchor, first_weight, second_weight, step_size):
    rows_here, cols_here, channels = anchor.shape
    widened = padded_2(anchor, (("rows", 0), ("cols", 1)), 2)
    slope_wide = apply_stencil(activate(widened), first_weight, rows_here + 2, cols_here + 2)
    middle_wide = widened[1:-1, 1:-1] + step_size * slope_wide
    row_global = lax.axis_index("rows") * rows_here - 1 + jnp.arange(rows_here + 2)
    col_global = lax.axis_index("cols") * cols_here - 1 + jnp.arange(cols_here + 2)
    inside_rows = (row_global >= 0) & (row_global < rows_here * lax.axis_size("rows"))
    inside_cols = (col_global >= 0) & (col_global < cols_here * lax.axis_size("cols"))
    inside = inside_rows[:, None] & inside_cols[None, :]
    second_act = jnp.where(inside[:, :, None], activate(middle_wide), jnp.zeros((), jnp.bfloat16))
    first_slope = slope_wide[1:-1, 1:-1]
    middle = middle_wide[1:-1, 1:-1]
    second_slope = apply_stencil(second_act, second_weight, rows_here, cols_here)
    ending = middle + step_size * second_slope
    return (first_slope, middle, ending)


def chain_on_device(section_states, weights):
    rows_here, cols_here, channels = section_states.shape[1:]
    ndepth = lax.axis_size("depth")
    position = lax.axis_index("depth")
    step_size = 2.0 / (2 * ndepth)
    first_weight = weights[0].reshape(9 * channels, channels)
    second_weight = weights[1].reshape(9 * channels, channels)
    anchor = section_states[0]
    first_slope, middle, ending = section_pass(anchor, first_weight, second_weight, step_size)
    jump = ending - (anchor + 2.0 * step_size * first_slope)

    def chain_turn(step_index, current):
        padded = padded_2(activate(current), (("rows", 0), ("cols", 1)), 1)
        advanced = (
            current
            + 2.0 * step_size * apply_stencil(padded, first_weight, rows_here, cols_here)
            + jump
        )
        shifted = shifted_2(advanced, "depth", 1)
        return jnp.where(position == 0, anchor, shifted)

    corrected = lax.fori_loop(0, ndepth - 1, chain_turn, anchor)
    final_slope, final_middle, final_ending = section_pass(
        corrected, first_weight, second_weight, step_size
    )
    fine_states = jnp.stack([final_middle, final_ending])
    return (fine_states, corrected[None])


def largest_divisor(total, limit):
    return max(n for n in range(1, limit + 1) if total % n == 0)


DIRECTIONS = ((-1, 0), (1, 0), (0, -1), (0, 1), (-1, -1), (-1, 1), (1, -1), (1, 1))


def cycle_kernel(
    sizes, x_hbm, w_hbm, act1, w_last, stage,
    w_first, base, mid, end, act0, inside, patches,
    flat, send_row, send_col, recv_row, recv_col, recv_corner,
    load_sem, send_sem, recv_sem, pass_send, pass_recv,
):
    nrows, ncols, step_size = sizes
    x = stage.at[2]
    w = (w_first, w_last)
    rows_here, cols_here, channels = x.shape
    halves = channels // LANES
    high, wide = rows_here + 2 * HALO, cols_here + 2 * HALO
    depth, row, col = lax.axis_index("depth"), lax.axis_index("rows"), lax.axis_index("cols")

    x_load = pltpu.make_async_copy(x_hbm.at[0], x, load_sem.at[0])
    w_loads = [pltpu.make_async_copy(w_hbm.at[k], w[k], load_sem.at[1 + k]) for k in range(2)]

    barrier = pltpu.get_barrier_semaphore()

    def neighbour(step):
        there_row, there_col = row + step[0], col + step[1]
        exists = (there_row >= 0) & (there_row < nrows) & (there_col >= 0) & (there_col < ncols)
        return exists, (depth, there_row, there_col)

    @pl.when(depth == 0)
    def _():
        x_load.start()

    for copy in w_loads:
        copy.start()
    pl.semaphore_signal(barrier, inc=1, device_id=(1 - depth, row, col), device_id_type=MESH)

    @pl.when(depth == 0)
    def _():
        for step in DIRECTIONS:
            exists, target = neighbour(step)

            @pl.when(exists)
            def _():
                pl.semaphore_signal(barrier, inc=1, device_id=target, device_id_type=MESH)

    def halves_of(c):
        return pl.ds(c * LANES, LANES)

    def silu(u):
        half = 0.5 * u
        return half + half * jnp.tanh(half)

    def masked_silu(u, first_row):
        half = 0.5 * u
        kept = half * inside[pl.ds(first_row, u.shape[0])]
        return kept + kept * jnp.tanh(half)

    def mark_inside(k, _):
        i = lax.broadcasted_iota(jnp.int32, (1, wide, LANES), 0) + (row * rows_here - HALO + k)
        j = lax.broadcasted_iota(jnp.int32, (1, wide, LANES), 1) + (col * cols_here - HALO)
        held = (i >= 0) & (i < nrows * rows_here) & (j >= 0) & (j < ncols * cols_here)
        inside[pl.ds(k, 1)] = jnp.where(held, 1.0, 0.0)
        return 0

    lax.fori_loop(0, high, mark_inside, 0, unroll=4)

    def slopes(act, layer, groups):
        m = sum(n for _, n in groups) * wide
        for a in range(3):
            for b in range(3):
                for c in range(halves):
                    filled = 0
                    for first_row, n in groups:
                        window = act[c, pl.ds(first_row + a - 1, n), b : b + wide, :]
                        patches[filled : filled + n * wide, pl.ds((a * 3 + b) * channels + c * LANES, LANES)] = (
                            window.reshape(n * wide, LANES).astype(jnp.bfloat16)
                        )
                        filled += n * wide
        acc = jnp.dot(patches[0:m, :], w[layer][...], preferred_element_type=jnp.float32)
        rises = []
        filled = 0
        for _, n in groups:
            rise = step_size * acc[filled : filled + n * wide]
            rises.append(
                [rise[:, c * LANES : (c + 1) * LANES].reshape(n, wide, LANES) for c in range(halves)]
            )
            filled += n * wide
        return rises

    def stage_interior(state, slot):
        def body(i, _):
            for c in range(halves):
                stage[slot, i, :, halves_of(c)] = state[c, i + HALO, HALO : HALO + cols_here, :]
            return 0

        lax.fori_loop(0, rows_here, body, 0, unroll=4)

    end_rows = high - 4
    piece = largest_divisor(end_rows, 9)
    pieces = end_rows // piece

    def hand_over(k):
        rows = pl.ds(2 + k * piece, piece)
        return pltpu.make_async_remote_copy(
            src_ref=end.at[:, rows], dst_ref=end.at[:, rows],
            send_sem=pass_send.at[k], recv_sem=pass_recv.at[k],
            device_id=(1 - depth, row, col), device_id_type=MESH,
        )

    def first_layer(source, groups):
        for (at, n), rise in zip(groups, slopes(act0, 0, groups)):
            for c in range(halves):
                u = source[c, pl.ds(at, n)] + rise[c]
                mid[c, pl.ds(at, n)] = u
                act1[c, pl.ds(at, n), 1 : 1 + wide, :] = masked_silu(u, at)

    @pl.when(depth == 0)
    def _():
        def clear(i, _):
            for c in range(halves):
                base[c, pl.ds(i, 1)] = jnp.zeros((1, wide, LANES), jnp.float32)
                act0[c, pl.ds(i, 1)] = jnp.zeros((1,) + act0.shape[2:], jnp.float32)
            return 0

        lax.fori_loop(0, high, clear, 0, unroll=4)
        x_load.wait()
        for side in range(2):
            rows_from = 0 if side == 0 else rows_here - HALO
            cols_from = 0 if side == 0 else cols_here - HALO
            send_row[side] = (
                x[rows_from : rows_from + HALO].reshape(HALO * cols_here, channels).astype(jnp.bfloat16)
            )
            for i in range(rows_here):
                for c in range(halves):
                    flat[side, c, i * HALO : (i + 1) * HALO, :] = x[
                        i, cols_from : cols_from + HALO, c * LANES : (c + 1) * LANES
                    ]
            for c in range(halves):
                send_col[side, :, halves_of(c)] = flat[side, c].astype(jnp.bfloat16)
        peers = jnp.int32(1)
        for step in DIRECTIONS:
            exists, target = neighbour(step)
            peers = peers + jnp.where(exists, 1, 0)
        pl.semaphore_wait(barrier, peers)

        corner = HALO * HALO
        copies = []
        for k, (dr, dc) in enumerate(DIRECTIONS):
            exists, target = neighbour((dr, dc))
            if dc == 0:
                side = (dr + 1) // 2
                src, dst = send_row.at[side], recv_row.at[1 - side]
            elif dr == 0:
                side = (dc + 1) // 2
                src, dst = send_col.at[side], recv_col.at[1 - side]
            else:
                side = (dc + 1) // 2
                from_row = 0 if dr < 0 else (rows_here - HALO) * HALO
                src = send_col.at[side, pl.ds(from_row, corner)]
                dst = recv_corner.at[(1 - dr) // 2, (1 - dc) // 2]
            opposite = DIRECTIONS.index((-dr, -dc))
            copy = pltpu.make_async_remote_copy(
                src_ref=src, dst_ref=dst, send_sem=send_sem.at[k], recv_sem=recv_sem.at[opposite],
                device_id=target, device_id_type=MESH,
            )
            arrival = pltpu.make_async_remote_copy(
                src_ref=src,
                dst_ref=(
                    recv_row.at[(dr + 1) // 2] if dc == 0
                    else recv_col.at[(dc + 1) // 2] if dr == 0
                    else recv_corner.at[(dr + 1) // 2, (dc + 1) // 2]
                ),
                send_sem=send_sem.at[k], recv_sem=recv_sem.at[k],
                device_id=target, device_id_type=MESH,
            )
            copies.append((exists, copy, arrival))
        order = (4, 5, 6, 7, 2, 3, 0, 1)
        for k in order:
            exists, copy, arrival = copies[k]
            pl.when(exists)(copy.start)

        def place(i, _):
            for c in range(halves):
                u = x[i, :, halves_of(c)]
                base[c, i + HALO, HALO : HALO + cols_here, :] = u
                act0[c, i + HALO, HALO + 1 : HALO + 1 + cols_here, :] = silu(u)
            return 0

        lax.fori_loop(0, rows_here, place, 0, unroll=4)

        def put(c, i, j, u, act):
            base[c, i, j : j + u.shape[0], :] = u
            act0[c, i, j + 1 : j + 1 + u.shape[0], :] = act

        def take(k):
            exists, copy, arrival = copies[k]
            dr, dc = DIRECTIONS[k]

            @pl.when(exists)
            def _(arrival=arrival, dr=dr, dc=dc):
                arrival.wait_recv()
                top = {-1: 0, 0: HALO, 1: high - HALO}[dr]
                left = {-1: 0, 0: HALO, 1: wide - HALO}[dc]
                for c in range(halves):
                    if dr == 0:
                        side = (dc + 1) // 2
                        u = recv_col[side, :, halves_of(c)].astype(jnp.float32)
                        flat[0, c] = u
                        flat[1, c] = silu(u)
                        for i in range(rows_here):
                            part = slice(i * HALO, (i + 1) * HALO)
                            put(c, top + i, left, flat[0, c, part, :], flat[1, c, part, :])
                        continue
                    if dc == 0:
                        u = recv_row[(dr + 1) // 2, :, halves_of(c)].astype(jnp.float32)
                    else:
                        u = recv_corner[(dr + 1) // 2, (dc + 1) // 2, :, halves_of(c)].astype(jnp.float32)
                    act, n = silu(u), u.shape[0] // HALO
                    for i in range(HALO):
                        part = slice(i * n, (i + 1) * n)
                        put(c, top + i, left, u[part], act[part])

        w_loads[0].wait()
        take(2)
        take(3)
        inner = rows_here - 2
        step = largest_divisor(inner, 15)

        def inner_rows(k, _):
            first_layer(base, [(HALO + 1 + k * step, step)])
            return 0

        lax.fori_loop(0, inner // step, inner_rows, 0)
        for k in (0, 1, 4, 5, 6, 7):
            take(k)
        first_layer(base, [(1, HALO), (high - HALO - 1, HALO)])
        stage_interior(mid, 0)
        w_loads[1].wait()

        def second(k, _):
            at = 2 + k * piece
            rise = slopes(act1, 1, [(at, piece)])[0]
            for c in range(halves):
                end[c, pl.ds(at, piece)] = mid[c, pl.ds(at, piece)] + rise[c]
            hand_over(k).start()
            return 0

        lax.fori_loop(0, pieces, second, 0)
        stage_interior(end, 1)
        for exists, copy, arrival in copies:

            @pl.when(exists)
            def _(copy=copy):
                copy.wait_send()

        def sent(k, _):
            hand_over(k).wait_send()
            return 0

        lax.fori_loop(0, pieces, sent, 0)

    @pl.when(depth == 1)
    def _():
        pl.semaphore_wait(barrier, 1)

        w_loads[0].wait()

        def received(k, _):
            hand_over(k).wait_recv()
            at = 2 + k * piece
            for c in range(halves):
                u = end[c, pl.ds(at, piece)]
                act0[c, pl.ds(at, piece), 1 : 1 + wide, :] = masked_silu(u, at)
            first_layer(end, [(at - 1, piece)])
            return 0

        lax.fori_loop(0, pieces, received, 0)
        stage_interior(end, 2)
        stage_interior(mid, 0)
        w_loads[1].wait()


def last_kernel(
    step_size, act, w, stage, fine_hbm, coarse_hbm, patches, ending, store_sem, piece_sem
):
    _, rows_here, cols_here, channels = stage.shape
    halves = channels // LANES
    depth = lax.axis_index("depth")
    pieces = piece_sem.shape[0]
    n = rows_here // pieces
    m = n * cols_here

    def store(slot, ref):
        return pltpu.make_async_copy(stage.at[slot], ref, store_sem.at[slot])

    coarse_store = store(2, coarse_hbm.at[0])
    first_store = store(0, fine_hbm.at[0])
    coarse_store.start()
    first_store.start()

    @pl.when(depth == 0)
    def _():
        second_store = store(1, fine_hbm.at[1])
        second_store.start()
        second_store.wait()

    @pl.when(depth == 1)
    def _():
        def piece_store(k):
            rows = pl.ds(k * n, n)
            return pltpu.make_async_copy(ending.at[rows], fine_hbm.at[1, rows], piece_sem.at[k])

        def last(k):
            at = k * n
            for a in range(3):
                for b in range(3):
                    for c in range(halves):
                        window = act[c, pl.ds(at + HALO + a - 1, n), HALO + b : HALO + b + cols_here, :]
                        patches[k % 2, :, pl.ds((a * 3 + b) * channels + c * LANES, LANES)] = (
                            window.reshape(m, LANES).astype(jnp.bfloat16)
                        )
            acc = jnp.dot(patches[k % 2], w[...], preferred_element_type=jnp.float32)
            ending[pl.ds(at, n)] = stage[0, pl.ds(at, n)] + step_size * acc.reshape(n, cols_here, channels)
            piece_store(k).start()

        for k in range(pieces):
            last(k)
        for k in range(pieces):
            piece_store(k).wait()

    coarse_store.wait()
    first_store.wait()


def two_sections(section_states, weights):
    _, rows_here, cols_here, channels = section_states.shape
    halves = channels // LANES
    high, wide = rows_here + 2 * HALO, cols_here + 2 * HALO
    act_wide = -(-(wide + 2) // 8) * 8
    pieces = (high - 4) // largest_divisor(high - 4, 9)
    sizes = (lax.axis_size("rows"), lax.axis_size("cols"), 2.0 / (2 * lax.axis_size("depth")))
    f32, bf16, vmem = jnp.float32, jnp.bfloat16, pltpu.VMEM
    state = vmem((halves, high, wide, LANES), f32)
    act = vmem((halves, high, act_wide, LANES), f32)
    most = max(largest_divisor(rows_here - 2, 15), 2 * HALO, largest_divisor(high - 4, 9))
    most_pixels = most * wide
    flat_weights = weights.reshape(2, 9 * channels, channels)
    any_space, in_vmem = pl.BlockSpec(memory_space=pl.ANY), pl.BlockSpec(memory_space=vmem)
    act_last, w_last, stage = pl.pallas_call(
        functools.partial(cycle_kernel, sizes),
        out_shape=(
            act,
            vmem((9 * channels, channels), bf16),
            vmem((3, rows_here, cols_here, channels), f32),
        ),
        in_specs=[pl.BlockSpec(memory_space=pltpu.HBM)] * 2,
        out_specs=[in_vmem] * 3,
        scratch_shapes=[
            vmem((9 * channels, channels), bf16),
            state, state, state, act,
            vmem((high, wide, LANES), f32),
            vmem((-(-most_pixels // 16) * 16, 9 * channels), bf16),
            vmem((2, halves, rows_here * HALO, LANES), f32),
            vmem((2, HALO * cols_here, channels), bf16),
            vmem((2, rows_here * HALO, channels), bf16),
            vmem((2, HALO * cols_here, channels), bf16),
            vmem((2, rows_here * HALO, channels), bf16),
            vmem((2, 2, HALO * HALO, channels), bf16),
            pltpu.SemaphoreType.DMA((3,)),
            pltpu.SemaphoreType.DMA((8,)),
            pltpu.SemaphoreType.DMA((8,)),
            pltpu.SemaphoreType.DMA((pieces,)),
            pltpu.SemaphoreType.DMA((pieces,)),
        ],
        compiler_params=pltpu.CompilerParams(
            collective_id=0, has_side_effects=True, vmem_limit_bytes=LIMIT
        ),
    )(
        pltpu.with_memory_space_constraint(section_states, pltpu.HBM),
        pltpu.with_memory_space_constraint(flat_weights, pltpu.HBM),
    )
    last_pieces = rows_here // largest_divisor(rows_here, 8)
    return pl.pallas_call(
        functools.partial(last_kernel, sizes[2]),
        out_shape=(
            jax.ShapeDtypeStruct((2, rows_here, cols_here, channels), f32),
            jax.ShapeDtypeStruct((1, rows_here, cols_here, channels), f32),
        ),
        in_specs=[in_vmem] * 3,
        out_specs=[any_space] * 2,
        scratch_shapes=[
            vmem((2, rows_here // last_pieces * cols_here, 9 * channels), bf16),
            vmem((rows_here, cols_here, channels), f32),
            pltpu.SemaphoreType.DMA((3,)),
            pltpu.SemaphoreType.DMA((last_pieces,)),
        ],
        compiler_params=pltpu.CompilerParams(vmem_limit_bytes=LIMIT),
    )(act_last, w_last, stage)


def on_device(section_states, weights):
    _, rows_here, cols_here, channels = section_states.shape
    tiles = rows_here % 8 == 0 and cols_here % 8 == 0 and channels % LANES == 0
    if lax.axis_size("depth") == 2 and tiles and min(rows_here, cols_here) >= HALO:
        return two_sections(section_states, weights)
    return chain_on_device(section_states, weights)


def solution(mesh):
    in_specs = (P("depth", "rows", "cols", None), P("depth", None, None, None, None))
    out_specs = (P("depth", "rows", "cols", None), P("depth", "rows", "cols", None))
    return jax.shard_map(
        on_device, mesh=mesh, in_specs=in_specs, out_specs=out_specs, check_vma=False
    )
```

```python
import functools

import jax
import jax.numpy as jnp
from jax import lax
from jax.experimental import pallas as pl
from jax.experimental.pallas import tpu as pltpu
from jax.sharding import PartitionSpec as P

MESH = pl.DeviceIdType.MESH
HALO = 4
LANES = 128
LIMIT = 32 * 1024 * 1024


def padded_2(shard, sides, width):
    for axis, dim in sides:
        size, length = (lax.axis_size(axis), shard.shape[dim])
        up = [(i, (i + 1) % size) for i in range(size - 1)]
        down = [(j, i) for i, j in up]
        last = lax.slice_in_dim(shard, length - width, length, axis=dim)
        initial = lax.slice_in_dim(shard, 0, width, axis=dim)
        before = lax.ppermute(last, axis, up)
        after = lax.ppermute(initial, axis, down)
        shard = jnp.concatenate([before, shard, after], axis=dim)
    return shard


def shifted_2(block, axis, distance):
    devices = range(lax.axis_size(axis))
    route = [(i - distance, i) for i in devices if i - distance in devices]
    return lax.ppermute(block, axis, route)


def activate(field):
    return jax.nn.silu(field).astype(jnp.bfloat16)


def apply_stencil(padded, flat_weight, out_rows, out_cols):
    channels = padded.shape[2]
    patches = jnp.concatenate(
        [
            padded[shift_row : shift_row + out_rows, shift_col : shift_col + out_cols]
            for shift_row in range(3)
            for shift_col in range(3)
        ],
        axis=2,
    )
    summed = jnp.dot(
        patches.reshape(out_rows * out_cols, 9 * channels),
        flat_weight,
        preferred_element_type=jnp.float32,
    )
    return summed.reshape(out_rows, out_cols, channels)


def section_pass(anchor, first_weight, second_weight, step_size):
    rows_here, cols_here, channels = anchor.shape
    widened = padded_2(anchor, (("rows", 0), ("cols", 1)), 2)
    slope_wide = apply_stencil(activate(widened), first_weight, rows_here + 2, cols_here + 2)
    middle_wide = widened[1:-1, 1:-1] + step_size * slope_wide
    row_global = lax.axis_index("rows") * rows_here - 1 + jnp.arange(rows_here + 2)
    col_global = lax.axis_index("cols") * cols_here - 1 + jnp.arange(cols_here + 2)
    inside_rows = (row_global >= 0) & (row_global < rows_here * lax.axis_size("rows"))
    inside_cols = (col_global >= 0) & (col_global < cols_here * lax.axis_size("cols"))
    inside = inside_rows[:, None] & inside_cols[None, :]
    second_act = jnp.where(inside[:, :, None], activate(middle_wide), jnp.zeros((), jnp.bfloat16))
    first_slope = slope_wide[1:-1, 1:-1]
    middle = middle_wide[1:-1, 1:-1]
    second_slope = apply_stencil(second_act, second_weight, rows_here, cols_here)
    ending = middle + step_size * second_slope
    return (first_slope, middle, ending)


def chain_on_device(section_states, weights):
    rows_here, cols_here, channels = section_states.shape[1:]
    ndepth = lax.axis_size("depth")
    position = lax.axis_index("depth")
    step_size = 2.0 / (2 * ndepth)
    first_weight = weights[0].reshape(9 * channels, channels)
    second_weight = weights[1].reshape(9 * channels, channels)
    anchor = section_states[0]
    first_slope, middle, ending = section_pass(anchor, first_weight, second_weight, step_size)
    jump = ending - (anchor + 2.0 * step_size * first_slope)

    def chain_turn(step_index, current):
        padded = padded_2(activate(current), (("rows", 0), ("cols", 1)), 1)
        advanced = (
            current
            + 2.0 * step_size * apply_stencil(padded, first_weight, rows_here, cols_here)
            + jump
        )
        shifted = shifted_2(advanced, "depth", 1)
        return jnp.where(position == 0, anchor, shifted)

    corrected = lax.fori_loop(0, ndepth - 1, chain_turn, anchor)
    final_slope, final_middle, final_ending = section_pass(
        corrected, first_weight, second_weight, step_size
    )
    fine_states = jnp.stack([final_middle, final_ending])
    return (fine_states, corrected[None])


def largest_divisor(total, limit):
    return max(n for n in range(1, limit + 1) if total % n == 0)


DIRECTIONS = ((-1, 0), (1, 0), (0, -1), (0, 1), (-1, -1), (-1, 1), (1, -1), (1, 1))


def cycle_kernel(
    sizes, x_hbm, w_hbm, act1, w_last, stage,
    w_first, base, mid, end, act0, inside,
    flat, send_row, send_col, recv_row, recv_col, recv_corner,
    load_sem, send_sem, recv_sem, pass_send, pass_recv,
):
    nrows, ncols, step_size = sizes
    x = stage.at[2]
    w = (w_first, w_last)
    rows_here, cols_here, channels = x.shape
    halves = channels // LANES
    high, wide = rows_here + 2 * HALO, cols_here + 2 * HALO
    depth, row, col = lax.axis_index("depth"), lax.axis_index("rows"), lax.axis_index("cols")

    x_load = pltpu.make_async_copy(x_hbm.at[0], x, load_sem.at[0])
    w_loads = [pltpu.make_async_copy(w_hbm.at[k], w[k], load_sem.at[1 + k]) for k in range(2)]

    barrier = pltpu.get_barrier_semaphore()

    def neighbour(step):
        there_row, there_col = row + step[0], col + step[1]
        exists = (there_row >= 0) & (there_row < nrows) & (there_col >= 0) & (there_col < ncols)
        return exists, (depth, there_row, there_col)

    @pl.when(depth == 0)
    def _():
        x_load.start()

    for copy in w_loads:
        copy.start()
    pl.semaphore_signal(barrier, inc=1, device_id=(1 - depth, row, col), device_id_type=MESH)

    @pl.when(depth == 0)
    def _():
        for step in DIRECTIONS:
            exists, target = neighbour(step)

            @pl.when(exists)
            def _():
                pl.semaphore_signal(barrier, inc=1, device_id=target, device_id_type=MESH)

    def halves_of(c):
        return pl.ds(c * LANES, LANES)

    def silu(u):
        half = 0.5 * u
        return half + half * jnp.tanh(half)

    def masked_silu(u, first_row):
        half = 0.5 * u
        kept = half * inside[pl.ds(first_row, u.shape[0])]
        return kept + kept * jnp.tanh(half)

    def mark_inside(k, _):
        i = lax.broadcasted_iota(jnp.int32, (1, wide, LANES), 0) + (row * rows_here - HALO + k)
        j = lax.broadcasted_iota(jnp.int32, (1, wide, LANES), 1) + (col * cols_here - HALO)
        held = (i >= 0) & (i < nrows * rows_here) & (j >= 0) & (j < ncols * cols_here)
        inside[pl.ds(k, 1)] = jnp.where(held, 1.0, 0.0)
        return 0

    lax.fori_loop(0, high, mark_inside, 0, unroll=4)

    def slopes(act, layer, groups):
        lhs = []
        for a in range(3):
            for b in range(3):
                for c in range(halves):
                    parts = [
                        act[c, pl.ds(first_row + a - 1, n), b : b + wide, :]
                        .reshape(n * wide, LANES).astype(jnp.bfloat16)
                        for first_row, n in groups
                    ]
                    lhs.append(parts[0] if len(parts) == 1 else jnp.concatenate(parts, axis=0))
        acc = jnp.dot(jnp.concatenate(lhs, axis=1), w[layer][...], preferred_element_type=jnp.float32)
        rises = []
        filled = 0
        for _, n in groups:
            rise = step_size * acc[filled : filled + n * wide]
            rises.append(
                [rise[:, c * LANES : (c + 1) * LANES].reshape(n, wide, LANES) for c in range(halves)]
            )
            filled += n * wide
        return rises

    def stage_interior(state, slot):
        def body(i, _):
            for c in range(halves):
                stage[slot, i, :, halves_of(c)] = state[c, i + HALO, HALO : HALO + cols_here, :]
            return 0

        lax.fori_loop(0, rows_here, body, 0, unroll=4)

    end_rows = high - 4
    piece = largest_divisor(end_rows, 9)
    pieces = end_rows // piece

    def hand_over(k):
        rows = pl.ds(2 + k * piece, piece)
        return pltpu.make_async_remote_copy(
            src_ref=end.at[:, rows], dst_ref=end.at[:, rows],
            send_sem=pass_send.at[k], recv_sem=pass_recv.at[k],
            device_id=(1 - depth, row, col), device_id_type=MESH,
        )

    def first_layer(source, groups):
        for (at, n), rise in zip(groups, slopes(act0, 0, groups)):
            for c in range(halves):
                u = source[c, pl.ds(at, n)] + rise[c]
                mid[c, pl.ds(at, n)] = u
                act1[c, pl.ds(at, n), 1 : 1 + wide, :] = masked_silu(u, at)

    @pl.when(depth == 0)
    def _():
        def clear(i, _):
            for c in range(halves):
                base[c, pl.ds(i, 1)] = jnp.zeros((1, wide, LANES), jnp.float32)
                act0[c, pl.ds(i, 1)] = jnp.zeros((1,) + act0.shape[2:], jnp.float32)
            return 0

        lax.fori_loop(0, high, clear, 0, unroll=4)
        x_load.wait()
        for side in range(2):
            rows_from = 0 if side == 0 else rows_here - HALO
            cols_from = 0 if side == 0 else cols_here - HALO
            send_row[side] = (
                x[rows_from : rows_from + HALO].reshape(HALO * cols_here, channels).astype(jnp.bfloat16)
            )
            for i in range(rows_here):
                for c in range(halves):
                    flat[side, c, i * HALO : (i + 1) * HALO, :] = x[
                        i, cols_from : cols_from + HALO, c * LANES : (c + 1) * LANES
                    ]
            for c in range(halves):
                send_col[side, :, halves_of(c)] = flat[side, c].astype(jnp.bfloat16)
        peers = jnp.int32(1)
        for step in DIRECTIONS:
            exists, target = neighbour(step)
            peers = peers + jnp.where(exists, 1, 0)
        pl.semaphore_wait(barrier, peers)

        corner = HALO * HALO
        copies = []
        for k, (dr, dc) in enumerate(DIRECTIONS):
            exists, target = neighbour((dr, dc))
            if dc == 0:
                side = (dr + 1) // 2
                src, dst = send_row.at[side], recv_row.at[1 - side]
            elif dr == 0:
                side = (dc + 1) // 2
                src, dst = send_col.at[side], recv_col.at[1 - side]
            else:
                side = (dc + 1) // 2
                from_row = 0 if dr < 0 else (rows_here - HALO) * HALO
                src = send_col.at[side, pl.ds(from_row, corner)]
                dst = recv_corner.at[(1 - dr) // 2, (1 - dc) // 2]
            opposite = DIRECTIONS.index((-dr, -dc))
            copy = pltpu.make_async_remote_copy(
                src_ref=src, dst_ref=dst, send_sem=send_sem.at[k], recv_sem=recv_sem.at[opposite],
                device_id=target, device_id_type=MESH,
            )
            arrival = pltpu.make_async_remote_copy(
                src_ref=src,
                dst_ref=(
                    recv_row.at[(dr + 1) // 2] if dc == 0
                    else recv_col.at[(dc + 1) // 2] if dr == 0
                    else recv_corner.at[(dr + 1) // 2, (dc + 1) // 2]
                ),
                send_sem=send_sem.at[k], recv_sem=recv_sem.at[k],
                device_id=target, device_id_type=MESH,
            )
            copies.append((exists, copy, arrival))
        order = (4, 5, 6, 7, 2, 3, 0, 1)
        for k in order:
            exists, copy, arrival = copies[k]
            pl.when(exists)(copy.start)

        def place(i, _):
            for c in range(halves):
                u = x[i, :, halves_of(c)]
                base[c, i + HALO, HALO : HALO + cols_here, :] = u
                act0[c, i + HALO, HALO + 1 : HALO + 1 + cols_here, :] = silu(u)
            return 0

        lax.fori_loop(0, rows_here, place, 0, unroll=4)

        def put(c, i, j, u, act):
            base[c, i, j : j + u.shape[0], :] = u
            act0[c, i, j + 1 : j + 1 + u.shape[0], :] = act

        def take(k):
            exists, copy, arrival = copies[k]
            dr, dc = DIRECTIONS[k]

            @pl.when(exists)
            def _(arrival=arrival, dr=dr, dc=dc):
                arrival.wait_recv()
                top = {-1: 0, 0: HALO, 1: high - HALO}[dr]
                left = {-1: 0, 0: HALO, 1: wide - HALO}[dc]
                for c in range(halves):
                    if dr == 0:
                        side = (dc + 1) // 2
                        u = recv_col[side, :, halves_of(c)].astype(jnp.float32)
                        flat[0, c] = u
                        flat[1, c] = silu(u)
                        for i in range(rows_here):
                            part = slice(i * HALO, (i + 1) * HALO)
                            put(c, top + i, left, flat[0, c, part, :], flat[1, c, part, :])
                        continue
                    if dc == 0:
                        u = recv_row[(dr + 1) // 2, :, halves_of(c)].astype(jnp.float32)
                    else:
                        u = recv_corner[(dr + 1) // 2, (dc + 1) // 2, :, halves_of(c)].astype(jnp.float32)
                    act, n = silu(u), u.shape[0] // HALO
                    for i in range(HALO):
                        part = slice(i * n, (i + 1) * n)
                        put(c, top + i, left, u[part], act[part])

        w_loads[0].wait()
        for k in (2, 3, 0, 1, 4, 5, 6, 7):
            take(k)
        first_layer(base, [(1, high - 2)])
        stage_interior(mid, 0)
        w_loads[1].wait()

        def second(k, _):
            at = 2 + k * piece
            rise = slopes(act1, 1, [(at, piece)])[0]
            for c in range(halves):
                end[c, pl.ds(at, piece)] = mid[c, pl.ds(at, piece)] + rise[c]
            hand_over(k).start()
            return 0

        lax.fori_loop(0, pieces, second, 0)
        stage_interior(end, 1)
        for exists, copy, arrival in copies:

            @pl.when(exists)
            def _(copy=copy):
                copy.wait_send()

        def sent(k, _):
            hand_over(k).wait_send()
            return 0

        lax.fori_loop(0, pieces, sent, 0)

    @pl.when(depth == 1)
    def _():
        pl.semaphore_wait(barrier, 1)

        w_loads[0].wait()

        def received(k, _):
            hand_over(k).wait_recv()
            at = 2 + k * piece
            for c in range(halves):
                u = end[c, pl.ds(at, piece)]
                act0[c, pl.ds(at, piece), 1 : 1 + wide, :] = masked_silu(u, at)
            first_layer(end, [(at - 1, piece)])
            return 0

        lax.fori_loop(0, pieces, received, 0)
        stage_interior(end, 2)
        stage_interior(mid, 0)
        w_loads[1].wait()


def last_kernel(
    step_size, act, w, stage, fine_hbm, coarse_hbm, ending, store_sem, piece_sem
):
    _, rows_here, cols_here, channels = stage.shape
    halves = channels // LANES
    depth = lax.axis_index("depth")
    pieces = piece_sem.shape[0]
    n = rows_here // pieces
    m = n * cols_here

    def store(slot, ref):
        return pltpu.make_async_copy(stage.at[slot], ref, store_sem.at[slot])

    coarse_store = store(2, coarse_hbm.at[0])
    first_store = store(0, fine_hbm.at[0])
    coarse_store.start()
    first_store.start()

    @pl.when(depth == 0)
    def _():
        second_store = store(1, fine_hbm.at[1])
        second_store.start()
        second_store.wait()

    @pl.when(depth == 1)
    def _():
        def piece_store(k):
            rows = pl.ds(k * n, n)
            return pltpu.make_async_copy(ending.at[rows], fine_hbm.at[1, rows], piece_sem.at[k])

        def last(k):
            at = k * n
            lhs = [
                act[c, pl.ds(at + HALO + a - 1, n), HALO + b : HALO + b + cols_here, :]
                .reshape(m, LANES).astype(jnp.bfloat16)
                for a in range(3) for b in range(3) for c in range(halves)
            ]
            acc = jnp.dot(jnp.concatenate(lhs, axis=1), w[...], preferred_element_type=jnp.float32)
            ending[pl.ds(at, n)] = stage[0, pl.ds(at, n)] + step_size * acc.reshape(n, cols_here, channels)
            piece_store(k).start()

        for k in range(pieces):
            last(k)
        for k in range(pieces):
            piece_store(k).wait()

    coarse_store.wait()
    first_store.wait()


def two_sections(section_states, weights):
    _, rows_here, cols_here, channels = section_states.shape
    halves = channels // LANES
    high, wide = rows_here + 2 * HALO, cols_here + 2 * HALO
    act_wide = -(-(wide + 2) // 8) * 8
    pieces = (high - 4) // largest_divisor(high - 4, 9)
    sizes = (lax.axis_size("rows"), lax.axis_size("cols"), 2.0 / (2 * lax.axis_size("depth")))
    f32, bf16, vmem = jnp.float32, jnp.bfloat16, pltpu.VMEM
    state = vmem((halves, high, wide, LANES), f32)
    act = vmem((halves, high, act_wide, LANES), f32)
    flat_weights = weights.reshape(2, 9 * channels, channels)
    any_space, in_vmem = pl.BlockSpec(memory_space=pl.ANY), pl.BlockSpec(memory_space=vmem)
    act_last, w_last, stage = pl.pallas_call(
        functools.partial(cycle_kernel, sizes),
        out_shape=(
            act,
            vmem((9 * channels, channels), bf16),
            vmem((3, rows_here, cols_here, channels), f32),
        ),
        in_specs=[pl.BlockSpec(memory_space=pltpu.HBM)] * 2,
        out_specs=[in_vmem] * 3,
        scratch_shapes=[
            vmem((9 * channels, channels), bf16),
            state, state, state, act,
            vmem((high, wide, LANES), f32),
            vmem((2, halves, rows_here * HALO, LANES), f32),
            vmem((2, HALO * cols_here, channels), bf16),
            vmem((2, rows_here * HALO, channels), bf16),
            vmem((2, HALO * cols_here, channels), bf16),
            vmem((2, rows_here * HALO, channels), bf16),
            vmem((2, 2, HALO * HALO, channels), bf16),
            pltpu.SemaphoreType.DMA((3,)),
            pltpu.SemaphoreType.DMA((8,)),
            pltpu.SemaphoreType.DMA((8,)),
            pltpu.SemaphoreType.DMA((pieces,)),
            pltpu.SemaphoreType.DMA((pieces,)),
        ],
        compiler_params=pltpu.CompilerParams(
            collective_id=0, has_side_effects=True, vmem_limit_bytes=LIMIT
        ),
    )(
        pltpu.with_memory_space_constraint(section_states, pltpu.HBM),
        pltpu.with_memory_space_constraint(flat_weights, pltpu.HBM),
    )
    last_pieces = rows_here // largest_divisor(rows_here, 8)
    return pl.pallas_call(
        functools.partial(last_kernel, sizes[2]),
        out_shape=(
            jax.ShapeDtypeStruct((2, rows_here, cols_here, channels), f32),
            jax.ShapeDtypeStruct((1, rows_here, cols_here, channels), f32),
        ),
        in_specs=[in_vmem] * 3,
        out_specs=[any_space] * 2,
        scratch_shapes=[
            vmem((rows_here, cols_here, channels), f32),
            pltpu.SemaphoreType.DMA((3,)),
            pltpu.SemaphoreType.DMA((last_pieces,)),
        ],
        compiler_params=pltpu.CompilerParams(vmem_limit_bytes=LIMIT),
    )(act_last, w_last, stage)


def on_device(section_states, weights):
    _, rows_here, cols_here, channels = section_states.shape
    tiles = rows_here % 8 == 0 and cols_here % 8 == 0 and channels % LANES == 0
    if lax.axis_size("depth") == 2 and tiles and min(rows_here, cols_here) >= HALO:
        return two_sections(section_states, weights)
    return chain_on_device(section_states, weights)


def solution(mesh):
    in_specs = (P("depth", "rows", "cols", None), P("depth", None, None, None, None))
    out_specs = (P("depth", "rows", "cols", None), P("depth", "rows", "cols", None))
    return jax.shard_map(
        on_device, mesh=mesh, in_specs=in_specs, out_specs=out_specs, check_vma=False
    )
```

```python
import functools

import jax
import jax.numpy as jnp
from jax import lax
from jax.experimental import pallas as pl
from jax.experimental.pallas import tpu as pltpu
from jax.sharding import PartitionSpec as P

MESH = pl.DeviceIdType.MESH
HALO = 4
LANES = 128
LIMIT = 32 * 1024 * 1024


def padded_2(shard, sides, width):
    for axis, dim in sides:
        size, length = (lax.axis_size(axis), shard.shape[dim])
        up = [(i, (i + 1) % size) for i in range(size - 1)]
        down = [(j, i) for i, j in up]
        last = lax.slice_in_dim(shard, length - width, length, axis=dim)
        initial = lax.slice_in_dim(shard, 0, width, axis=dim)
        before = lax.ppermute(last, axis, up)
        after = lax.ppermute(initial, axis, down)
        shard = jnp.concatenate([before, shard, after], axis=dim)
    return shard


def shifted_2(block, axis, distance):
    devices = range(lax.axis_size(axis))
    route = [(i - distance, i) for i in devices if i - distance in devices]
    return lax.ppermute(block, axis, route)


def activate(field):
    return jax.nn.silu(field).astype(jnp.bfloat16)


def apply_stencil(padded, flat_weight, out_rows, out_cols):
    channels = padded.shape[2]
    patches = jnp.concatenate(
        [
            padded[shift_row : shift_row + out_rows, shift_col : shift_col + out_cols]
            for shift_row in range(3)
            for shift_col in range(3)
        ],
        axis=2,
    )
    summed = jnp.dot(
        patches.reshape(out_rows * out_cols, 9 * channels),
        flat_weight,
        preferred_element_type=jnp.float32,
    )
    return summed.reshape(out_rows, out_cols, channels)


def section_pass(anchor, first_weight, second_weight, step_size):
    rows_here, cols_here, channels = anchor.shape
    widened = padded_2(anchor, (("rows", 0), ("cols", 1)), 2)
    slope_wide = apply_stencil(activate(widened), first_weight, rows_here + 2, cols_here + 2)
    middle_wide = widened[1:-1, 1:-1] + step_size * slope_wide
    row_global = lax.axis_index("rows") * rows_here - 1 + jnp.arange(rows_here + 2)
    col_global = lax.axis_index("cols") * cols_here - 1 + jnp.arange(cols_here + 2)
    inside_rows = (row_global >= 0) & (row_global < rows_here * lax.axis_size("rows"))
    inside_cols = (col_global >= 0) & (col_global < cols_here * lax.axis_size("cols"))
    inside = inside_rows[:, None] & inside_cols[None, :]
    second_act = jnp.where(inside[:, :, None], activate(middle_wide), jnp.zeros((), jnp.bfloat16))
    first_slope = slope_wide[1:-1, 1:-1]
    middle = middle_wide[1:-1, 1:-1]
    second_slope = apply_stencil(second_act, second_weight, rows_here, cols_here)
    ending = middle + step_size * second_slope
    return (first_slope, middle, ending)


def chain_on_device(section_states, weights):
    rows_here, cols_here, channels = section_states.shape[1:]
    ndepth = lax.axis_size("depth")
    position = lax.axis_index("depth")
    step_size = 2.0 / (2 * ndepth)
    first_weight = weights[0].reshape(9 * channels, channels)
    second_weight = weights[1].reshape(9 * channels, channels)
    anchor = section_states[0]
    first_slope, middle, ending = section_pass(anchor, first_weight, second_weight, step_size)
    jump = ending - (anchor + 2.0 * step_size * first_slope)

    def chain_turn(step_index, current):
        padded = padded_2(activate(current), (("rows", 0), ("cols", 1)), 1)
        advanced = (
            current
            + 2.0 * step_size * apply_stencil(padded, first_weight, rows_here, cols_here)
            + jump
        )
        shifted = shifted_2(advanced, "depth", 1)
        return jnp.where(position == 0, anchor, shifted)

    corrected = lax.fori_loop(0, ndepth - 1, chain_turn, anchor)
    final_slope, final_middle, final_ending = section_pass(
        corrected, first_weight, second_weight, step_size
    )
    fine_states = jnp.stack([final_middle, final_ending])
    return (fine_states, corrected[None])


def largest_divisor(total, limit):
    return max(n for n in range(1, limit + 1) if total % n == 0)


DIRECTIONS = ((-1, 0), (1, 0), (0, -1), (0, 1), (-1, -1), (-1, 1), (1, -1), (1, 1))


def cycle_kernel(
    sizes, x_hbm, w_hbm, act1, w_last, stage,
    w_first, base, mid, end, act0, inside,
    flat, send_row, send_col, recv_row, recv_col, recv_corner,
    load_sem, send_sem, recv_sem, pass_send, pass_recv,
):
    nrows, ncols, step_size = sizes
    x = stage.at[2]
    w = (w_first, w_last)
    rows_here, cols_here, channels = x.shape
    halves = channels // LANES
    high, wide = rows_here + 2 * HALO, cols_here + 2 * HALO
    depth, row, col = lax.axis_index("depth"), lax.axis_index("rows"), lax.axis_index("cols")

    x_load = pltpu.make_async_copy(x_hbm.at[0], x, load_sem.at[0])
    w_loads = [pltpu.make_async_copy(w_hbm.at[k], w[k], load_sem.at[1 + k]) for k in range(2)]

    barrier = pltpu.get_barrier_semaphore()

    def neighbour(step):
        there_row, there_col = row + step[0], col + step[1]
        exists = (there_row >= 0) & (there_row < nrows) & (there_col >= 0) & (there_col < ncols)
        return exists, (depth, there_row, there_col)

    @pl.when(depth == 0)
    def _():
        x_load.start()

    for copy in w_loads:
        copy.start()
    pl.semaphore_signal(barrier, inc=1, device_id=(1 - depth, row, col), device_id_type=MESH)

    @pl.when(depth == 0)
    def _():
        for step in DIRECTIONS:
            exists, target = neighbour(step)

            @pl.when(exists)
            def _():
                pl.semaphore_signal(barrier, inc=1, device_id=target, device_id_type=MESH)

    def halves_of(c):
        return pl.ds(c * LANES, LANES)

    def silu(u):
        half = 0.5 * u
        return half + half * jnp.tanh(half)

    def masked_silu(u, first_row):
        half = 0.5 * u
        kept = half * inside[pl.ds(first_row, u.shape[0])]
        return kept + kept * jnp.tanh(half)

    def mark_inside(k, _):
        i = lax.broadcasted_iota(jnp.int32, (1, wide, LANES), 0) + (row * rows_here - HALO + k)
        j = lax.broadcasted_iota(jnp.int32, (1, wide, LANES), 1) + (col * cols_here - HALO)
        held = (i >= 0) & (i < nrows * rows_here) & (j >= 0) & (j < ncols * cols_here)
        inside[pl.ds(k, 1)] = jnp.where(held, 1.0, 0.0)
        return 0

    lax.fori_loop(0, high, mark_inside, 0, unroll=4)

    def slopes(act, layer, groups):
        lhs = []
        for a in range(3):
            for b in range(3):
                for c in range(halves):
                    parts = [
                        act[c, pl.ds(first_row + a - 1, n), b : b + wide, :]
                        .reshape(n * wide, LANES).astype(jnp.bfloat16)
                        for first_row, n in groups
                    ]
                    lhs.append(parts[0] if len(parts) == 1 else jnp.concatenate(parts, axis=0))
        acc = jnp.dot(jnp.concatenate(lhs, axis=1), w[layer][...], preferred_element_type=jnp.float32)
        rises = []
        filled = 0
        for _, n in groups:
            rise = step_size * acc[filled : filled + n * wide]
            rises.append(
                [rise[:, c * LANES : (c + 1) * LANES].reshape(n, wide, LANES) for c in range(halves)]
            )
            filled += n * wide
        return rises

    def stage_interior(state, slot):
        def body(i, _):
            for c in range(halves):
                stage[slot, i, :, halves_of(c)] = state[c, i + HALO, HALO : HALO + cols_here, :]
            return 0

        lax.fori_loop(0, rows_here, body, 0, unroll=4)

    end_rows = high - 4
    piece = largest_divisor(end_rows, 9)
    pieces = end_rows // piece

    def hand_over(k):
        rows = pl.ds(2 + k * piece, piece)
        return pltpu.make_async_remote_copy(
            src_ref=end.at[:, rows], dst_ref=end.at[:, rows],
            send_sem=pass_send.at[k], recv_sem=pass_recv.at[k],
            device_id=(1 - depth, row, col), device_id_type=MESH,
        )

    def first_layer(source, groups):
        for (at, n), rise in zip(groups, slopes(act0, 0, groups)):
            for c in range(halves):
                u = source[c, pl.ds(at, n)] + rise[c]
                mid[c, pl.ds(at, n)] = u
                act1[c, pl.ds(at, n), 1 : 1 + wide, :] = masked_silu(u, at)

    @pl.when(depth == 0)
    def _():
        def clear(i, _):
            for c in range(halves):
                base[c, pl.ds(i, 1)] = jnp.zeros((1, wide, LANES), jnp.float32)
                act0[c, pl.ds(i, 1)] = jnp.zeros((1,) + act0.shape[2:], jnp.float32)
            return 0

        lax.fori_loop(0, high, clear, 0, unroll=4)
        x_load.wait()
        for side in range(2):
            rows_from = 0 if side == 0 else rows_here - HALO
            cols_from = 0 if side == 0 else cols_here - HALO
            send_row[side] = (
                x[rows_from : rows_from + HALO].reshape(HALO * cols_here, channels).astype(jnp.bfloat16)
            )
            for i in range(rows_here):
                for c in range(halves):
                    flat[side, c, i * HALO : (i + 1) * HALO, :] = x[
                        i, cols_from : cols_from + HALO, c * LANES : (c + 1) * LANES
                    ]
            for c in range(halves):
                send_col[side, :, halves_of(c)] = flat[side, c].astype(jnp.bfloat16)
        peers = jnp.int32(1)
        for step in DIRECTIONS:
            exists, target = neighbour(step)
            peers = peers + jnp.where(exists, 1, 0)
        pl.semaphore_wait(barrier, peers)

        corner = HALO * HALO
        copies = []
        for k, (dr, dc) in enumerate(DIRECTIONS):
            exists, target = neighbour((dr, dc))
            if dc == 0:
                side = (dr + 1) // 2
                src, dst = send_row.at[side], recv_row.at[1 - side]
            elif dr == 0:
                side = (dc + 1) // 2
                src, dst = send_col.at[side], recv_col.at[1 - side]
            else:
                side = (dc + 1) // 2
                from_row = 0 if dr < 0 else (rows_here - HALO) * HALO
                src = send_col.at[side, pl.ds(from_row, corner)]
                dst = recv_corner.at[(1 - dr) // 2, (1 - dc) // 2]
            opposite = DIRECTIONS.index((-dr, -dc))
            copy = pltpu.make_async_remote_copy(
                src_ref=src, dst_ref=dst, send_sem=send_sem.at[k], recv_sem=recv_sem.at[opposite],
                device_id=target, device_id_type=MESH,
            )
            arrival = pltpu.make_async_remote_copy(
                src_ref=src,
                dst_ref=(
                    recv_row.at[(dr + 1) // 2] if dc == 0
                    else recv_col.at[(dc + 1) // 2] if dr == 0
                    else recv_corner.at[(dr + 1) // 2, (dc + 1) // 2]
                ),
                send_sem=send_sem.at[k], recv_sem=recv_sem.at[k],
                device_id=target, device_id_type=MESH,
            )
            copies.append((exists, copy, arrival))
        order = (2, 3, 4, 5, 6, 7, 0, 1)
        for k in order:
            exists, copy, arrival = copies[k]
            pl.when(exists)(copy.start)

        def place(i, _):
            for c in range(halves):
                u = x[i, :, halves_of(c)]
                base[c, i + HALO, HALO : HALO + cols_here, :] = u
                act0[c, i + HALO, HALO + 1 : HALO + 1 + cols_here, :] = silu(u)
            return 0

        lax.fori_loop(0, rows_here, place, 0, unroll=4)

        def put(c, i, j, u, act):
            base[c, i, j : j + u.shape[0], :] = u
            act0[c, i, j + 1 : j + 1 + u.shape[0], :] = act

        def take(k):
            exists, copy, arrival = copies[k]
            dr, dc = DIRECTIONS[k]

            @pl.when(exists)
            def _(arrival=arrival, dr=dr, dc=dc):
                arrival.wait_recv()
                top = {-1: 0, 0: HALO, 1: high - HALO}[dr]
                left = {-1: 0, 0: HALO, 1: wide - HALO}[dc]
                for c in range(halves):
                    if dr == 0:
                        side = (dc + 1) // 2
                        u = recv_col[side, :, halves_of(c)].astype(jnp.float32)
                        flat[0, c] = u
                        flat[1, c] = silu(u)
                        for i in range(rows_here):
                            part = slice(i * HALO, (i + 1) * HALO)
                            put(c, top + i, left, flat[0, c, part, :], flat[1, c, part, :])
                        continue
                    if dc == 0:
                        u = recv_row[(dr + 1) // 2, :, halves_of(c)].astype(jnp.float32)
                    else:
                        u = recv_corner[(dr + 1) // 2, (dc + 1) // 2, :, halves_of(c)].astype(jnp.float32)
                    act, n = silu(u), u.shape[0] // HALO
                    for i in range(HALO):
                        part = slice(i * n, (i + 1) * n)
                        put(c, top + i, left, u[part], act[part])

        w_loads[0].wait()
        for k in (0, 1, 4, 5, 6, 7, 2, 3):
            take(k)
        first_layer(base, [(1, high - 2)])
        w_loads[1].wait()

        def second(k, _):
            at = 2 + k * piece
            rise = slopes(act1, 1, [(at, piece)])[0]
            for c in range(halves):
                end[c, pl.ds(at, piece)] = mid[c, pl.ds(at, piece)] + rise[c]
            hand_over(k).start()
            return 0

        lax.fori_loop(0, pieces, second, 0)
        stage_interior(mid, 0)
        stage_interior(end, 1)
        for exists, copy, arrival in copies:

            @pl.when(exists)
            def _(copy=copy):
                copy.wait_send()

        def sent(k, _):
            hand_over(k).wait_send()
            return 0

        lax.fori_loop(0, pieces, sent, 0)

    @pl.when(depth == 1)
    def _():
        pl.semaphore_wait(barrier, 1)

        w_loads[0].wait()

        def received(k, _):
            hand_over(k).wait_recv()
            at = 2 + k * piece
            for c in range(halves):
                u = end[c, pl.ds(at, piece)]
                act0[c, pl.ds(at, piece), 1 : 1 + wide, :] = masked_silu(u, at)
            first_layer(end, [(at - 1, piece)])
            return 0

        lax.fori_loop(0, pieces, received, 0)
        stage_interior(end, 2)
        stage_interior(mid, 0)
        w_loads[1].wait()


def last_kernel(
    step_size, act, w, stage, fine_hbm, coarse_hbm, ending, store_sem, piece_sem
):
    _, rows_here, cols_here, channels = stage.shape
    halves = channels // LANES
    depth = lax.axis_index("depth")
    pieces = piece_sem.shape[0]
    n = rows_here // pieces
    m = n * cols_here

    def store(slot, ref):
        return pltpu.make_async_copy(stage.at[slot], ref, store_sem.at[slot])

    coarse_store = store(2, coarse_hbm.at[0])
    first_store = store(0, fine_hbm.at[0])
    coarse_store.start()
    first_store.start()

    @pl.when(depth == 0)
    def _():
        second_store = store(1, fine_hbm.at[1])
        second_store.start()
        second_store.wait()

    @pl.when(depth == 1)
    def _():
        def piece_store(k):
            rows = pl.ds(k * n, n)
            return pltpu.make_async_copy(ending.at[rows], fine_hbm.at[1, rows], piece_sem.at[k])

        def last(k):
            at = k * n
            lhs = [
                act[c, pl.ds(at + HALO + a - 1, n), HALO + b : HALO + b + cols_here, :]
                .reshape(m, LANES).astype(jnp.bfloat16)
                for a in range(3) for b in range(3) for c in range(halves)
            ]
            acc = jnp.dot(jnp.concatenate(lhs, axis=1), w[...], preferred_element_type=jnp.float32)
            ending[pl.ds(at, n)] = stage[0, pl.ds(at, n)] + step_size * acc.reshape(n, cols_here, channels)
            piece_store(k).start()

        for k in range(pieces):
            last(k)
        for k in range(pieces):
            piece_store(k).wait()

    coarse_store.wait()
    first_store.wait()


def two_sections(section_states, weights):
    _, rows_here, cols_here, channels = section_states.shape
    halves = channels // LANES
    high, wide = rows_here + 2 * HALO, cols_here + 2 * HALO
    act_wide = -(-(wide + 2) // 8) * 8
    pieces = (high - 4) // largest_divisor(high - 4, 9)
    sizes = (lax.axis_size("rows"), lax.axis_size("cols"), 2.0 / (2 * lax.axis_size("depth")))
    f32, bf16, vmem = jnp.float32, jnp.bfloat16, pltpu.VMEM
    state = vmem((halves, high, wide, LANES), f32)
    act = vmem((halves, high, act_wide, LANES), f32)
    flat_weights = weights.reshape(2, 9 * channels, channels)
    any_space, in_vmem = pl.BlockSpec(memory_space=pl.ANY), pl.BlockSpec(memory_space=vmem)
    act_last, w_last, stage = pl.pallas_call(
        functools.partial(cycle_kernel, sizes),
        out_shape=(
            act,
            vmem((9 * channels, channels), bf16),
            vmem((3, rows_here, cols_here, channels), f32),
        ),
        in_specs=[pl.BlockSpec(memory_space=pltpu.HBM)] * 2,
        out_specs=[in_vmem] * 3,
        scratch_shapes=[
            vmem((9 * channels, channels), bf16),
            state, state, state, act,
            vmem((high, wide, LANES), f32),
            vmem((2, halves, rows_here * HALO, LANES), f32),
            vmem((2, HALO * cols_here, channels), bf16),
            vmem((2, rows_here * HALO, channels), bf16),
            vmem((2, HALO * cols_here, channels), bf16),
            vmem((2, rows_here * HALO, channels), bf16),
            vmem((2, 2, HALO * HALO, channels), bf16),
            pltpu.SemaphoreType.DMA((3,)),
            pltpu.SemaphoreType.DMA((8,)),
            pltpu.SemaphoreType.DMA((8,)),
            pltpu.SemaphoreType.DMA((pieces,)),
            pltpu.SemaphoreType.DMA((pieces,)),
        ],
        compiler_params=pltpu.CompilerParams(
            collective_id=0, has_side_effects=True, vmem_limit_bytes=LIMIT
        ),
    )(
        pltpu.with_memory_space_constraint(section_states, pltpu.HBM),
        pltpu.with_memory_space_constraint(flat_weights, pltpu.HBM),
    )
    last_pieces = rows_here // largest_divisor(rows_here, 8)
    return pl.pallas_call(
        functools.partial(last_kernel, sizes[2]),
        out_shape=(
            jax.ShapeDtypeStruct((2, rows_here, cols_here, channels), f32),
            jax.ShapeDtypeStruct((1, rows_here, cols_here, channels), f32),
        ),
        in_specs=[in_vmem] * 3,
        out_specs=[any_space] * 2,
        scratch_shapes=[
            vmem((rows_here, cols_here, channels), f32),
            pltpu.SemaphoreType.DMA((3,)),
            pltpu.SemaphoreType.DMA((last_pieces,)),
        ],
        compiler_params=pltpu.CompilerParams(vmem_limit_bytes=LIMIT),
    )(act_last, w_last, stage)


def on_device(section_states, weights):
    _, rows_here, cols_here, channels = section_states.shape
    tiles = rows_here % 8 == 0 and cols_here % 8 == 0 and channels % LANES == 0
    if lax.axis_size("depth") == 2 and tiles and min(rows_here, cols_here) >= HALO:
        return two_sections(section_states, weights)
    return chain_on_device(section_states, weights)


def solution(mesh):
    in_specs = (P("depth", "rows", "cols", None), P("depth", None, None, None, None))
    out_specs = (P("depth", "rows", "cols", None), P("depth", "rows", "cols", None))
    return jax.shard_map(
        on_device, mesh=mesh, in_specs=in_specs, out_specs=out_specs, check_vma=False
    )
```

```python
import functools

import jax
import jax.numpy as jnp
from jax import lax
from jax.experimental import pallas as pl
from jax.experimental.pallas import tpu as pltpu
from jax.sharding import PartitionSpec as P

MESH = pl.DeviceIdType.MESH
HALO = 4
LANES = 128
LIMIT = 32 * 1024 * 1024


def padded_2(shard, sides, width):
    for axis, dim in sides:
        size, length = (lax.axis_size(axis), shard.shape[dim])
        up = [(i, (i + 1) % size) for i in range(size - 1)]
        down = [(j, i) for i, j in up]
        last = lax.slice_in_dim(shard, length - width, length, axis=dim)
        initial = lax.slice_in_dim(shard, 0, width, axis=dim)
        before = lax.ppermute(last, axis, up)
        after = lax.ppermute(initial, axis, down)
        shard = jnp.concatenate([before, shard, after], axis=dim)
    return shard


def shifted_2(block, axis, distance):
    devices = range(lax.axis_size(axis))
    route = [(i - distance, i) for i in devices if i - distance in devices]
    return lax.ppermute(block, axis, route)


def activate(field):
    return jax.nn.silu(field).astype(jnp.bfloat16)


def apply_stencil(padded, flat_weight, out_rows, out_cols):
    channels = padded.shape[2]
    patches = jnp.concatenate(
        [
            padded[shift_row : shift_row + out_rows, shift_col : shift_col + out_cols]
            for shift_row in range(3)
            for shift_col in range(3)
        ],
        axis=2,
    )
    summed = jnp.dot(
        patches.reshape(out_rows * out_cols, 9 * channels),
        flat_weight,
        preferred_element_type=jnp.float32,
    )
    return summed.reshape(out_rows, out_cols, channels)


def section_pass(anchor, first_weight, second_weight, step_size):
    rows_here, cols_here, channels = anchor.shape
    widened = padded_2(anchor, (("rows", 0), ("cols", 1)), 2)
    slope_wide = apply_stencil(activate(widened), first_weight, rows_here + 2, cols_here + 2)
    middle_wide = widened[1:-1, 1:-1] + step_size * slope_wide
    row_global = lax.axis_index("rows") * rows_here - 1 + jnp.arange(rows_here + 2)
    col_global = lax.axis_index("cols") * cols_here - 1 + jnp.arange(cols_here + 2)
    inside_rows = (row_global >= 0) & (row_global < rows_here * lax.axis_size("rows"))
    inside_cols = (col_global >= 0) & (col_global < cols_here * lax.axis_size("cols"))
    inside = inside_rows[:, None] & inside_cols[None, :]
    second_act = jnp.where(inside[:, :, None], activate(middle_wide), jnp.zeros((), jnp.bfloat16))
    first_slope = slope_wide[1:-1, 1:-1]
    middle = middle_wide[1:-1, 1:-1]
    second_slope = apply_stencil(second_act, second_weight, rows_here, cols_here)
    ending = middle + step_size * second_slope
    return (first_slope, middle, ending)


def chain_on_device(section_states, weights):
    rows_here, cols_here, channels = section_states.shape[1:]
    ndepth = lax.axis_size("depth")
    position = lax.axis_index("depth")
    step_size = 2.0 / (2 * ndepth)
    first_weight = weights[0].reshape(9 * channels, channels)
    second_weight = weights[1].reshape(9 * channels, channels)
    anchor = section_states[0]
    first_slope, middle, ending = section_pass(anchor, first_weight, second_weight, step_size)
    jump = ending - (anchor + 2.0 * step_size * first_slope)

    def chain_turn(step_index, current):
        padded = padded_2(activate(current), (("rows", 0), ("cols", 1)), 1)
        advanced = (
            current
            + 2.0 * step_size * apply_stencil(padded, first_weight, rows_here, cols_here)
            + jump
        )
        shifted = shifted_2(advanced, "depth", 1)
        return jnp.where(position == 0, anchor, shifted)

    corrected = lax.fori_loop(0, ndepth - 1, chain_turn, anchor)
    final_slope, final_middle, final_ending = section_pass(
        corrected, first_weight, second_weight, step_size
    )
    fine_states = jnp.stack([final_middle, final_ending])
    return (fine_states, corrected[None])


def largest_divisor(total, limit):
    return max(n for n in range(1, limit + 1) if total % n == 0)


DIRECTIONS = ((-1, 0), (1, 0), (0, -1), (0, 1), (-1, -1), (-1, 1), (1, -1), (1, 1))


def cycle_kernel(
    sizes, x_hbm, w_hbm, act1, w_last, stage,
    w_first, base, mid, end, act0, inside,
    flat, send_row, send_col, recv_row, recv_col, recv_corner,
    load_sem, send_sem, recv_sem, pass_send, pass_recv,
):
    nrows, ncols, step_size = sizes
    x = stage.at[2]
    w = (w_first, w_last)
    rows_here, cols_here, channels = x.shape
    halves = channels // LANES
    high, wide = rows_here + 2 * HALO, cols_here + 2 * HALO
    depth, row, col = lax.axis_index("depth"), lax.axis_index("rows"), lax.axis_index("cols")

    x_load = pltpu.make_async_copy(x_hbm.at[0], x, load_sem.at[0])
    w_loads = [pltpu.make_async_copy(w_hbm.at[k], w[k], load_sem.at[1 + k]) for k in range(2)]

    barrier = pltpu.get_barrier_semaphore()

    def neighbour(step):
        there_row, there_col = row + step[0], col + step[1]
        exists = (there_row >= 0) & (there_row < nrows) & (there_col >= 0) & (there_col < ncols)
        return exists, (depth, there_row, there_col)

    @pl.when(depth == 0)
    def _():
        x_load.start()

    for copy in w_loads:
        copy.start()
    pl.semaphore_signal(barrier, inc=1, device_id=(1 - depth, row, col), device_id_type=MESH)

    @pl.when(depth == 0)
    def _():
        for step in DIRECTIONS:
            exists, target = neighbour(step)

            @pl.when(exists)
            def _():
                pl.semaphore_signal(barrier, inc=1, device_id=target, device_id_type=MESH)

    def halves_of(c):
        return pl.ds(c * LANES, LANES)

    def silu(u):
        half = 0.5 * u
        return half + half * jnp.tanh(half)

    def masked_silu(u, first_row):
        half = 0.5 * u
        kept = half * inside[pl.ds(first_row, u.shape[0])]
        return kept + kept * jnp.tanh(half)

    def mark_inside(k, _):
        i = lax.broadcasted_iota(jnp.int32, (1, wide, LANES), 0) + (row * rows_here - HALO + k)
        j = lax.broadcasted_iota(jnp.int32, (1, wide, LANES), 1) + (col * cols_here - HALO)
        held = (i >= 0) & (i < nrows * rows_here) & (j >= 0) & (j < ncols * cols_here)
        inside[pl.ds(k, 1)] = jnp.where(held, 1.0, 0.0)
        return 0

    lax.fori_loop(0, high, mark_inside, 0, unroll=4)

    def slopes(act, layer, groups):
        lhs = []
        for a in range(3):
            for b in range(3):
                for c in range(halves):
                    parts = [
                        act[c, pl.ds(first_row + a - 1, n), b : b + wide, :]
                        .reshape(n * wide, LANES).astype(jnp.bfloat16)
                        for first_row, n in groups
                    ]
                    lhs.append(parts[0] if len(parts) == 1 else jnp.concatenate(parts, axis=0))
        acc = jnp.dot(jnp.concatenate(lhs, axis=1), w[layer][...], preferred_element_type=jnp.float32)
        rises = []
        filled = 0
        for _, n in groups:
            rise = step_size * acc[filled : filled + n * wide]
            rises.append(
                [rise[:, c * LANES : (c + 1) * LANES].reshape(n, wide, LANES) for c in range(halves)]
            )
            filled += n * wide
        return rises

    def stage_interior(state, slot):
        def body(i, _):
            for c in range(halves):
                stage[slot, i, :, halves_of(c)] = state[c, i + HALO, HALO : HALO + cols_here, :]
            return 0

        lax.fori_loop(0, rows_here, body, 0, unroll=4)

    end_rows = high - 4
    piece = largest_divisor(end_rows, 9)
    pieces = end_rows // piece

    def hand_over(k):
        rows = pl.ds(2 + k * piece, piece)
        return pltpu.make_async_remote_copy(
            src_ref=end.at[:, rows], dst_ref=end.at[:, rows],
            send_sem=pass_send.at[k], recv_sem=pass_recv.at[k],
            device_id=(1 - depth, row, col), device_id_type=MESH,
        )

    def first_layer(source, groups):
        for (at, n), rise in zip(groups, slopes(act0, 0, groups)):
            for c in range(halves):
                u = source[c, pl.ds(at, n)] + rise[c]
                mid[c, pl.ds(at, n)] = u
                act1[c, pl.ds(at, n), 1 : 1 + wide, :] = masked_silu(u, at)

    @pl.when(depth == 0)
    def _():
        def clear(i, _):
            for c in range(halves):
                base[c, pl.ds(i, 1)] = jnp.zeros((1, wide, LANES), jnp.float32)
                act0[c, pl.ds(i, 1)] = jnp.zeros((1,) + act0.shape[2:], jnp.float32)
            return 0

        lax.fori_loop(0, high, clear, 0, unroll=4)
        x_load.wait()
        for side in range(2):
            rows_from = 0 if side == 0 else rows_here - HALO
            cols_from = 0 if side == 0 else cols_here - HALO
            send_row[side] = (
                x[rows_from : rows_from + HALO].reshape(HALO * cols_here, channels).astype(jnp.bfloat16)
            )
            for i in range(rows_here):
                for c in range(halves):
                    flat[side, c, i * HALO : (i + 1) * HALO, :] = x[
                        i, cols_from : cols_from + HALO, c * LANES : (c + 1) * LANES
                    ]
            for c in range(halves):
                send_col[side, :, halves_of(c)] = flat[side, c].astype(jnp.bfloat16)
        peers = jnp.int32(1)
        for step in DIRECTIONS:
            exists, target = neighbour(step)
            peers = peers + jnp.where(exists, 1, 0)
        pl.semaphore_wait(barrier, peers)

        corner = HALO * HALO
        copies = []
        for k, (dr, dc) in enumerate(DIRECTIONS):
            exists, target = neighbour((dr, dc))
            if dc == 0:
                side = (dr + 1) // 2
                src, dst = send_row.at[side], recv_row.at[1 - side]
            elif dr == 0:
                side = (dc + 1) // 2
                src, dst = send_col.at[side], recv_col.at[1 - side]
            else:
                side = (dc + 1) // 2
                from_row = 0 if dr < 0 else (rows_here - HALO) * HALO
                src = send_col.at[side, pl.ds(from_row, corner)]
                dst = recv_corner.at[(1 - dr) // 2, (1 - dc) // 2]
            opposite = DIRECTIONS.index((-dr, -dc))
            copy = pltpu.make_async_remote_copy(
                src_ref=src, dst_ref=dst, send_sem=send_sem.at[k], recv_sem=recv_sem.at[opposite],
                device_id=target, device_id_type=MESH,
            )
            arrival = pltpu.make_async_remote_copy(
                src_ref=src,
                dst_ref=(
                    recv_row.at[(dr + 1) // 2] if dc == 0
                    else recv_col.at[(dc + 1) // 2] if dr == 0
                    else recv_corner.at[(dr + 1) // 2, (dc + 1) // 2]
                ),
                send_sem=send_sem.at[k], recv_sem=recv_sem.at[k],
                device_id=target, device_id_type=MESH,
            )
            copies.append((exists, copy, arrival))
        order = (4, 5, 6, 7, 2, 3, 0, 1)
        for k in order:
            exists, copy, arrival = copies[k]
            pl.when(exists)(copy.start)

        def place(i, _):
            for c in range(halves):
                u = x[i, :, halves_of(c)]
                base[c, i + HALO, HALO : HALO + cols_here, :] = u
                act0[c, i + HALO, HALO + 1 : HALO + 1 + cols_here, :] = silu(u)
            return 0

        lax.fori_loop(0, rows_here, place, 0, unroll=4)

        def put(c, i, j, u, act):
            base[c, i, j : j + u.shape[0], :] = u
            act0[c, i, j + 1 : j + 1 + u.shape[0], :] = act

        def take(k):
            exists, copy, arrival = copies[k]
            dr, dc = DIRECTIONS[k]

            @pl.when(exists)
            def _(arrival=arrival, dr=dr, dc=dc):
                arrival.wait_recv()
                top = {-1: 0, 0: HALO, 1: high - HALO}[dr]
                left = {-1: 0, 0: HALO, 1: wide - HALO}[dc]
                for c in range(halves):
                    if dr == 0:
                        side = (dc + 1) // 2
                        u = recv_col[side, :, halves_of(c)].astype(jnp.float32)
                        flat[0, c] = u
                        flat[1, c] = silu(u)
                        for i in range(rows_here):
                            part = slice(i * HALO, (i + 1) * HALO)
                            put(c, top + i, left, flat[0, c, part, :], flat[1, c, part, :])
                        continue
                    if dc == 0:
                        u = recv_row[(dr + 1) // 2, :, halves_of(c)].astype(jnp.float32)
                    else:
                        u = recv_corner[(dr + 1) // 2, (dc + 1) // 2, :, halves_of(c)].astype(jnp.float32)
                    act, n = silu(u), u.shape[0] // HALO
                    for i in range(HALO):
                        part = slice(i * n, (i + 1) * n)
                        put(c, top + i, left, u[part], act[part])

        w_loads[0].wait()
        for k in (0, 1, 4, 5, 6, 7, 2, 3):
            take(k)
        first_layer(base, [(1, high - 2)])
        w_loads[1].wait()

        def second(k, _):
            at = 2 + k * piece
            rise = slopes(act1, 1, [(at, piece)])[0]
            for c in range(halves):
                end[c, pl.ds(at, piece)] = mid[c, pl.ds(at, piece)] + rise[c]
            hand_over(k).start()
            return 0

        lax.fori_loop(0, pieces, second, 0)
        stage_interior(mid, 0)
        stage_interior(end, 1)
        for exists, copy, arrival in copies:

            @pl.when(exists)
            def _(copy=copy):
                copy.wait_send()

        def sent(k, _):
            hand_over(k).wait_send()
            return 0

        lax.fori_loop(0, pieces, sent, 0)

    @pl.when(depth == 1)
    def _():
        pl.semaphore_wait(barrier, 1)

        w_loads[0].wait()

        def received(k, _):
            hand_over(k).wait_recv()
            at = 2 + k * piece
            for c in range(halves):
                u = end[c, pl.ds(at, piece)]
                act0[c, pl.ds(at, piece), 1 : 1 + wide, :] = masked_silu(u, at)
            first_layer(end, [(at - 1, piece)])
            return 0

        lax.fori_loop(0, pieces, received, 0)
        stage_interior(end, 2)
        stage_interior(mid, 0)
        w_loads[1].wait()


def last_kernel(
    step_size, act, w, stage, fine_hbm, coarse_hbm, ending, store_sem, piece_sem
):
    _, rows_here, cols_here, channels = stage.shape
    halves = channels // LANES
    depth = lax.axis_index("depth")
    pieces = piece_sem.shape[0]
    n = rows_here // pieces
    m = n * cols_here

    def store(slot, ref):
        return pltpu.make_async_copy(stage.at[slot], ref, store_sem.at[slot])

    coarse_store = store(2, coarse_hbm.at[0])
    first_store = store(0, fine_hbm.at[0])
    coarse_store.start()
    first_store.start()

    @pl.when(depth == 0)
    def _():
        second_store = store(1, fine_hbm.at[1])
        second_store.start()
        second_store.wait()

    @pl.when(depth == 1)
    def _():
        def piece_store(k):
            rows = pl.ds(k * n, n)
            return pltpu.make_async_copy(ending.at[rows], fine_hbm.at[1, rows], piece_sem.at[k])

        def last(k):
            at = k * n
            lhs = [
                act[c, pl.ds(at + HALO + a - 1, n), HALO + b : HALO + b + cols_here, :]
                .reshape(m, LANES).astype(jnp.bfloat16)
                for a in range(3) for b in range(3) for c in range(halves)
            ]
            acc = jnp.dot(jnp.concatenate(lhs, axis=1), w[...], preferred_element_type=jnp.float32)
            ending[pl.ds(at, n)] = stage[0, pl.ds(at, n)] + step_size * acc.reshape(n, cols_here, channels)
            piece_store(k).start()

        for k in range(pieces):
            last(k)
        for k in range(pieces):
            piece_store(k).wait()

    coarse_store.wait()
    first_store.wait()


def two_sections(section_states, weights):
    _, rows_here, cols_here, channels = section_states.shape
    halves = channels // LANES
    high, wide = rows_here + 2 * HALO, cols_here + 2 * HALO
    act_wide = -(-(wide + 2) // 8) * 8
    pieces = (high - 4) // largest_divisor(high - 4, 9)
    sizes = (lax.axis_size("rows"), lax.axis_size("cols"), 2.0 / (2 * lax.axis_size("depth")))
    f32, bf16, vmem = jnp.float32, jnp.bfloat16, pltpu.VMEM
    state = vmem((halves, high, wide, LANES), f32)
    act = vmem((halves, high, act_wide, LANES), f32)
    flat_weights = weights.reshape(2, 9 * channels, channels)
    any_space, in_vmem = pl.BlockSpec(memory_space=pl.ANY), pl.BlockSpec(memory_space=vmem)
    act_last, w_last, stage = pl.pallas_call(
        functools.partial(cycle_kernel, sizes),
        out_shape=(
            act,
            vmem((9 * channels, channels), bf16),
            vmem((3, rows_here, cols_here, channels), f32),
        ),
        in_specs=[pl.BlockSpec(memory_space=pltpu.HBM)] * 2,
        out_specs=[in_vmem] * 3,
        scratch_shapes=[
            vmem((9 * channels, channels), bf16),
            state, state, state, act,
            vmem((high, wide, LANES), f32),
            vmem((2, halves, rows_here * HALO, LANES), f32),
            vmem((2, HALO * cols_here, channels), bf16),
            vmem((2, rows_here * HALO, channels), bf16),
            vmem((2, HALO * cols_here, channels), bf16),
            vmem((2, rows_here * HALO, channels), bf16),
            vmem((2, 2, HALO * HALO, channels), bf16),
            pltpu.SemaphoreType.DMA((3,)),
            pltpu.SemaphoreType.DMA((8,)),
            pltpu.SemaphoreType.DMA((8,)),
            pltpu.SemaphoreType.DMA((pieces,)),
            pltpu.SemaphoreType.DMA((pieces,)),
        ],
        compiler_params=pltpu.CompilerParams(
            collective_id=0, has_side_effects=True, vmem_limit_bytes=LIMIT
        ),
    )(
        pltpu.with_memory_space_constraint(section_states, pltpu.HBM),
        pltpu.with_memory_space_constraint(flat_weights, pltpu.HBM),
    )
    last_pieces = rows_here // largest_divisor(rows_here, 8)
    return pl.pallas_call(
        functools.partial(last_kernel, sizes[2]),
        out_shape=(
            jax.ShapeDtypeStruct((2, rows_here, cols_here, channels), f32),
            jax.ShapeDtypeStruct((1, rows_here, cols_here, channels), f32),
        ),
        in_specs=[in_vmem] * 3,
        out_specs=[any_space] * 2,
        scratch_shapes=[
            vmem((rows_here, cols_here, channels), f32),
            pltpu.SemaphoreType.DMA((3,)),
            pltpu.SemaphoreType.DMA((last_pieces,)),
        ],
        compiler_params=pltpu.CompilerParams(vmem_limit_bytes=LIMIT),
    )(act_last, w_last, stage)


def on_device(section_states, weights):
    _, rows_here, cols_here, channels = section_states.shape
    tiles = rows_here % 8 == 0 and cols_here % 8 == 0 and channels % LANES == 0
    if lax.axis_size("depth") == 2 and tiles and min(rows_here, cols_here) >= HALO:
        return two_sections(section_states, weights)
    return chain_on_device(section_states, weights)


def solution(mesh):
    in_specs = (P("depth", "rows", "cols", None), P("depth", None, None, None, None))
    out_specs = (P("depth", "rows", "cols", None), P("depth", "rows", "cols", None))
    return jax.shard_map(
        on_device, mesh=mesh, in_specs=in_specs, out_specs=out_specs, check_vma=False
    )
```
